32 devices in a mesh: dp: 1 (over z), sp: 32 (over x, y, core).
Axes of the slice: x: 4, y: 4, z: 1, core: 2. Of those that a mesh axis runs over, the one named last changes fastest.
The devices are a block of a 4x4x8 slice.
Arguments:
- x: bfloat16 [4096, 4096], P(('dp', 'sp'))
- gain: bfloat16 [4096], replicated
- wq: bfloat16 [4096, 4096], replicated
- wk: bfloat16 [4096, 1024], replicated
- wv: bfloat16 [4096, 1024], replicated
- wo: bfloat16 [4096, 4096], replicated
Outputs:
- output: bfloat16 [4096, 4096], P(('dp', 'sp'))
All inputs are finite; a program needn't handle non-finite values.
Results may differ from the reference program's by a relative error of at most 0.012.
Values are sent between devices in bfloat16 or wider.
A program may use at most 768 MiB of HBM per device.

```python
import jax
import jax.numpy as jnp
from jax import lax

ROWS = 4096
D = 4096
HEADS = 32
KV_HEADS = 8
HEAD = 128
THETA = 10000


def setup_inputs(seed: int = 0, part: int = 0) -> dict:
    kx, kn, kq, kk, kv, ko = jax.random.split(jax.random.key(seed), 6)

    def weights(key, rows, columns):
        return jax.random.normal(key, (rows, columns), jnp.float32) * rows**-0.5

    drawn = {
        "x": jax.random.normal(jax.random.fold_in(kx, part), (ROWS, D), jnp.float32),
        "gain": 1 + 0.1 * jax.random.normal(kn, (D,), jnp.float32),
        "wq": 2 * weights(kq, D, HEADS * HEAD),
        "wk": 2 * weights(kk, D, KV_HEADS * HEAD),
        "wv": 4 * weights(kv, D, KV_HEADS * HEAD),
        "wo": weights(ko, HEADS * HEAD, D),
    }
    return {k: v.astype(jnp.bfloat16) for k, v in drawn.items()}


def normed(x, gain):
    wide = x.astype(jnp.float32)
    scale = lax.rsqrt(jnp.mean(wide * wide, -1, keepdims=True) + 1e-6)
    return (wide * scale * gain.astype(jnp.float32)).astype(jnp.bfloat16)


def turned(t, place, theta):
    half = t.shape[-1] // 2
    angle = place.astype(jnp.float32)[:, None] * theta ** (-jnp.arange(half, dtype=jnp.float32) / half)
    cos, sin = jnp.cos(angle)[:, None], jnp.sin(angle)[:, None]
    a, b = t[..., :half].astype(jnp.float32), t[..., half:].astype(jnp.float32)
    return jnp.concatenate([a * cos - b * sin, b * cos + a * sin], -1).astype(jnp.bfloat16)


def matmul(a, w):
    return jnp.dot(a, w, preferred_element_type=jnp.float32).astype(jnp.bfloat16)


def einsum(form, a, b):
    return jnp.einsum(form, a.astype(jnp.float32), b.astype(jnp.float32))


def attention(q, k, v):
    scores = einsum("tgsd,ugd->gstu", q, k) * q.shape[-1] ** -0.5
    token = jnp.arange(q.shape[0])
    scores = jnp.where(token[:, None] >= token, scores, -jnp.inf)
    weights = jax.nn.softmax(scores, -1).astype(jnp.bfloat16)
    return einsum("gstu,ugd->tgsd", weights, v).astype(jnp.bfloat16)


def reference(x, gain, wq, wk, wv, wo):
    a, place = normed(x, gain), jnp.arange(ROWS)
    q = turned(matmul(a, wq).reshape(ROWS, HEADS, HEAD), place, THETA).reshape(ROWS, KV_HEADS, -1, HEAD)
    k = turned(matmul(a, wk).reshape(ROWS, KV_HEADS, HEAD), place, THETA)
    v = matmul(a, wv).reshape(ROWS, KV_HEADS, HEAD)
    seen = attention(q, k, v).reshape(ROWS, HEADS * HEAD)
    return (x.astype(jnp.float32) + jnp.dot(seen, wo, preferred_element_type=jnp.float32)).astype(jnp.bfloat16)
```

```python
import functools

import jax
import jax.numpy as jnp
from jax import lax
from jax.experimental import pallas as pl
from jax.experimental.pallas import tpu as pltpu
from jax.sharding import PartitionSpec as P

HEAD = 128
THETA = 10000
CORES = 2
NEG = -1e30
HIDDEN = 2 * NEG
LOG2E = 1.4426950408889634
SLOTS = 4
WO_SLOTS = 6
MESH = pl.DeviceIdType.MESH


def _dot(a, b, ca=1, cb=0):
    return lax.dot_general(a, b, (((ca,), (cb,)), ((), ())), preferred_element_type=jnp.float32)


def _kernel(nx, ny, x_hbm, gain_ref, cos_ref, sin_ref, wq, wk, wv, wo, y_ref,
            xv, av, wbuf, wobuf, kvs, kvg, qs, qg, os, og, acc, top_s, mix_s,
            x_sem, w_sem, wo_sem, kv_send, kv_recv, y_send, y_recv, q_send, q_recv, o_send, o_recv):
    own, dim = xv.shape
    nu = nx * CORES
    group = qs.shape[2]
    reps = group // HEAD
    me = lax.axis_index("sp")
    x, y, c = lax.div(me, CORES * ny), lax.rem(lax.div(me, CORES), ny), lax.rem(me, CORES)
    u = x * CORES + c

    def dev(xx, yy, cc):
        return {"sp": (xx * ny + yy) * CORES + cc}

    def remote(src, dst, send, recv, to):
        return pltpu.make_async_remote_copy(src_ref=src, dst_ref=dst, send_sem=send, recv_sem=recv, device_id=to, device_id_type=MESH)

    def target(j):
        k = lax.rem(j + CORES, nu)
        return lax.rem(x + lax.div(k, CORES), nx), lax.rem(c + lax.rem(k, CORES), CORES)

    def load_kv(n):
        cols = pl.ds(pl.multiple_of(lax.rem(x + n + 1, nx) * (CORES * HEAD), CORES * HEAD), CORES * HEAD)
        wide = CORES * HEAD
        return [pltpu.make_async_copy(wk.at[:, cols], wbuf.at[n % SLOTS, :, pl.ds(0, wide)], w_sem.at[n % SLOTS, 0]),
                pltpu.make_async_copy(wv.at[:, cols], wbuf.at[n % SLOTS, :, pl.ds(wide, wide)], w_sem.at[n % SLOTS, 1])]

    def load_q(j):
        xx, cc = target(j)
        cols = pl.ds(pl.multiple_of((xx * CORES + cc) * group, group), group)
        slot = lax.rem(j + nx, SLOTS)
        return pltpu.make_async_copy(wq.at[:, cols], wbuf.at[slot], w_sem.at[slot, 0])

    def source(j):
        return lax.rem(x + j // CORES, nx) * CORES + lax.rem(c + j % CORES, CORES)

    def load_o(j):
        k = lax.rem(j, nu)
        head = lax.rem(x + lax.div(k, CORES), nx) * CORES + lax.rem(c + lax.rem(k, CORES), CORES)
        rows = pl.ds(pl.multiple_of(head * group, group), group)
        slot = lax.rem(j, WO_SLOTS)
        return pltpu.make_async_copy(wo.at[rows, :], wobuf.at[slot], wo_sem.at[slot])

    get_x = pltpu.make_async_copy(x_hbm, xv, x_sem)
    get_x.start()
    for n in range(SLOTS):
        for copy in load_kv(n):
            copy.start()

    barrier = pltpu.get_barrier_semaphore()
    peers = [dev(lax.rem(x + k // CORES, nx), y, lax.rem(c + k % CORES, CORES)) for k in range(1, nu)]
    peers += [dev(x, lax.rem(y + d, ny), c) for d in range(1, ny)]
    for peer in peers:
        pl.semaphore_signal(barrier, inc=1, device_id=peer, device_id_type=MESH)

    get_x.wait()
    wide = xv[...].astype(jnp.float32)
    scale = lax.rsqrt(jnp.mean(wide * wide, -1, keepdims=True) + 1e-6)
    av[...] = (wide * scale * gain_ref[...].astype(jnp.float32)).astype(jnp.bfloat16)
    pl.semaphore_wait(barrier, len(peers))

    def turn(t):
        t = t.astype(jnp.float32)
        return (t * cos_ref[...] + pltpu.roll(t, HEAD // 2, 1) * sin_ref[...]).astype(jnp.bfloat16)

    for n in range(nx):
        for copy in load_kv(n):
            copy.wait()
        both = _dot(av[...], wbuf[n % SLOTS]).astype(jnp.bfloat16)
        load_q(jnp.int32(n)).start()
        xx = lax.rem(x + n + 1, nx)
        for h in range(CORES):
            i = n * CORES + h
            kvs[i, :HEAD, :] = turn(both[:, h * HEAD : (h + 1) * HEAD])
            at = (CORES + h) * HEAD
            kvs[i, HEAD:, :] = both[:, at : at + HEAD].T
            there = remote(kvs.at[i], kvg.at[y * nu + u], kv_send.at[i], kv_recv.at[u], dev(xx, y, h))
            if n < nx - 1:
                there.start()
            else:
                here = pltpu.make_async_copy(kvs.at[i], kvg.at[y * nu + u], kv_recv.at[u])
                pl.when(c == h)(here.start)
                pl.when(c != h)(there.start)

    def passed(d, xx):
        block = kvg.at[pl.ds(y * nu + xx * CORES, CORES)]
        return remote(block, block, y_send.at[d - 1, xx], y_recv.at[d - 1, xx], dev(x, lax.rem(y + d, ny), c))

    def arrived(d, xx):
        block = kvg.at[pl.ds(lax.rem(y + ny - d, ny) * nu + xx * CORES, CORES)]
        return pltpu.make_async_copy(block, block, y_recv.at[d - 1, xx])

    def queries(j, _):
        load_q(j).wait()
        slot = lax.rem(j + nx, SLOTS)
        t = _dot(av[...], wbuf[slot]).astype(jnp.bfloat16)

        @pl.when(j + SLOTS < nu)
        def _():
            load_q(j + SLOTS).start()

        @pl.when(j + SLOTS >= nu)
        def _():
            load_o(j + SLOTS - nu).start()

        for s in range(reps):
            qs[j, :, s * HEAD : (s + 1) * HEAD] = turn(t[:, s * HEAD : (s + 1) * HEAD])
        xx, cc = target(j)
        mine = (xx == x) & (cc == c)
        here = pltpu.make_async_copy(qs.at[j], qg.at[u], q_recv.at[u])
        there = remote(qs.at[j], qg.at[u], q_send.at[j], q_recv.at[u], dev(xx, y, cc))
        pl.when(mine)(here.start)
        pl.when(jnp.logical_not(mine))(there.start)

        @pl.when(j < nx)
        def _():
            for h in range(CORES):
                block = kvg.at[y * nu + j * CORES + h]
                pltpu.make_async_copy(block, block, kv_recv.at[j * CORES + h]).wait()
            for d in range(1, ny):
                passed(d, j).start()

    lax.fori_loop(0, nu, queries, None)
    for j in range(nu - (nu - SLOTS), WO_SLOTS):
        load_o(jnp.int32(j)).start()

    e = HEAD**-0.5 * LOG2E
    strips = [(h, at) for h in range(CORES) for at in range(0, group, 2 * HEAD)]
    cols = 2 * HEAD

    def block(xx, slots, masked):
        bk = len(slots) * HEAD
        k = jnp.concatenate([kvg[i, :HEAD, :] for i in slots], axis=0)
        scores = []
        for h, at in strips:
            t = qg[xx * CORES + h, :, at : at + cols]
            t = jnp.concatenate([t[:, :HEAD], t[:, HEAD:]], axis=0)
            scores.append(_dot(k, t, 1, 1))
        weights, keeps = [], []
        for i, (h, _) in enumerate(strips):
            s = scores[i]
            if masked:
                query = h * HEAD + lax.rem(lax.broadcasted_iota(jnp.int32, (bk, cols), 1), HEAD)
                s = jnp.where(query >= lax.broadcasted_iota(jnp.int32, (bk, cols), 0), s, HIDDEN)
            old = top_s[i : i + 1, :]
            top = jnp.maximum(old, s.max(axis=0, keepdims=True))
            top_s[i : i + 1, :] = top
            weights.append(jnp.exp2((s - top) * e).astype(jnp.bfloat16))
            keeps.append(jnp.exp2((old - top) * e))
        v = jnp.concatenate([kvg[i, HEAD:, :] for i in slots], axis=1)
        v = jnp.concatenate([v, jnp.ones((8, bk), jnp.bfloat16)], axis=0)
        for i in range(len(strips)):
            mix_s[i] = mix_s[i] * keeps[i] + _dot(v, weights[i])

    def chunk(xx, _):
        for h in range(CORES):
            part = qg.at[xx * CORES + h]
            pltpu.make_async_copy(part, part, q_recv.at[xx * CORES + h]).wait()
        for d in range(1, ny):
            arrived(d, xx).wait()
        top_s[...] = jnp.full(top_s.shape, NEG, jnp.float32)
        mix_s[...] = jnp.zeros(mix_s.shape, jnp.float32)

        def whole(t, _):
            first = lax.rem(t, ny // 2) * (2 * nu) + lax.div(t, ny // 2) * CORES
            block(xx, [first + a * nu + h for a in range(2) for h in range(CORES)], False)

        lax.fori_loop(0, xx * (ny // 2), whole, None)
        lax.fori_loop(0, y, lambda t, _: block(xx, [t * nu + xx * CORES + h for h in range(CORES)], False), None)
        block(xx, [y * nu + xx * CORES + h for h in range(CORES)], True)

        for i, (h, at) in enumerate(strips):
            done = (mix_s[i, :HEAD, :] * (1 / mix_s[i, HEAD : HEAD + 1, :])).astype(jnp.bfloat16)
            for s in range(2):
                os[xx * CORES + h, :, at + s * HEAD : at + (s + 1) * HEAD] = done[:, s * HEAD : (s + 1) * HEAD].T
        for h in range(CORES):
            i = xx * CORES + h
            mine = (xx == x) & (c == h)
            here = pltpu.make_async_copy(os.at[i], og.at[u], o_recv.at[u])
            there = remote(os.at[i], og.at[u], o_send.at[i], o_recv.at[u], dev(xx, y, h))
            pl.when(mine)(here.start)
            pl.when(jnp.logical_not(mine))(there.start)

    lax.fori_loop(0, nx, chunk, None)

    step = min(dim, 1024)

    def project(j, _):
        k = lax.rem(j, nu)
        head = lax.rem(x + lax.div(k, CORES), nx) * CORES + lax.rem(c + lax.rem(k, CORES), CORES)
        part = og.at[head]
        pltpu.make_async_copy(part, part, o_recv.at[head]).wait()
        load_o(j).wait()
        slot = lax.rem(j, WO_SLOTS)

        def columns(n, _):
            at = pl.ds(pl.multiple_of(n * step, step), step)
            more = _dot(og[head], wobuf[slot, :, at])

            @pl.when(j == 0)
            def _():
                acc[:, at] = more

            @pl.when(j > 0)
            def _():
                acc[:, at] += more

        lax.fori_loop(0, dim // step, columns, None)

        @pl.when(j + WO_SLOTS < nu)
        def _():
            load_o(j + WO_SLOTS).start()

    lax.fori_loop(0, nu, project, None)
    y_ref[...] = (xv[...].astype(jnp.float32) + acc[...]).astype(jnp.bfloat16)

    for n in range(nx):
        for h in range(CORES):
            i = n * CORES + h
            wait = remote(kvs.at[i], kvg.at[y * nu + u], kv_send.at[i], kv_recv.at[u], dev(x, y, h)).wait_send
            if n < nx - 1:
                wait()
            else:
                pl.when(c != h)(wait)
    for xx in range(nx):
        for d in range(1, ny):
            passed(d, xx).wait_send()

    def left(j, _):
        xx, cc = target(j)
        mine = (xx == x) & (cc == c)
        pl.when(jnp.logical_not(mine))(remote(qs.at[j], qg.at[u], q_send.at[j], q_recv.at[u], dev(xx, y, cc)).wait_send)
        pl.when(j != u)(remote(os.at[j], og.at[u], o_send.at[j], o_recv.at[u], dev(xx, y, cc)).wait_send)

    lax.fori_loop(0, nu, left, None)


def solution(mesh):
    total = mesh.shape["sp"]

    def step(x, gain, wq, wk, wv, wo):
        own, dim = x.shape
        nu = wk.shape[1] // HEAD
        nx, ny = nu // CORES, total // nu
        group = wq.shape[1] // nu
        place = lax.axis_index("sp") * own + jnp.arange(own)
        half = HEAD // 2
        angle = place.astype(jnp.float32)[:, None] * THETA ** (-jnp.arange(half, dtype=jnp.float32) / half)
        cos, sin = jnp.cos(angle), jnp.sin(angle)
        cos, sin = jnp.concatenate([cos, cos], -1), jnp.concatenate([-sin, sin], -1)
        any_ = pl.BlockSpec(memory_space=pltpu.HBM)
        vmem = pl.BlockSpec(memory_space=pltpu.VMEM)
        low, wide = jnp.bfloat16, jnp.float32
        dma = pltpu.SemaphoreType.DMA
        strips = CORES * group // (2 * HEAD)
        return pl.pallas_call(
            functools.partial(_kernel, nx, ny),
            out_shape=jax.ShapeDtypeStruct((own, dim), low),
            in_specs=[any_, vmem, vmem, vmem, any_, any_, any_, any_],
            out_specs=vmem,
            scratch_shapes=[
                pltpu.VMEM((own, dim), low),
                pltpu.VMEM((own, dim), low),
                pltpu.VMEM((SLOTS, dim, group), low),
                pltpu.VMEM((WO_SLOTS, group, dim), low),
                pltpu.VMEM((nu, 2 * HEAD, own), low),
                pltpu.VMEM((ny * nu, 2 * HEAD, own), low),
                pltpu.VMEM((nu, own, group), low),
                pltpu.VMEM((nu, own, group), low),
                pltpu.VMEM((nu, own, group), low),
                pltpu.VMEM((nu, own, group), low),
                pltpu.VMEM((own, dim), wide),
                pltpu.VMEM((strips, 2 * HEAD), wide),
                pltpu.VMEM((strips, HEAD + 8, 2 * HEAD), wide),
                dma, dma((SLOTS, 2)), dma((WO_SLOTS,)),
                dma((nu,)), dma((nu,)), dma((ny - 1, nx)), dma((ny - 1, nx)),
                dma((nu,)), dma((nu,)), dma((nu,)), dma((nu,)),
            ],
            compiler_params=pltpu.CompilerParams(collective_id=0, has_side_effects=True, vmem_limit_bytes=63 * 2**20),
        )(x, gain[None], cos, sin, wq, wk, wv, wo)

    tokens, whole = P(("dp", "sp"), None), P(None, None)
    return jax.shard_map(
        step,
        mesh=mesh,
        in_specs=(tokens, P(None), whole, whole, whole, whole),
        out_specs=tokens,
        check_vma=False,
    )
```

```python
import functools
import math

import jax
import jax.numpy as jnp
from jax import lax
from jax.experimental import pallas as pl
from jax.experimental.pallas import tpu as pltpu
from jax.sharding import PartitionSpec as P

HEAD = 128
THETA = 10000
CORES = 2
NEG = -1e30
HIDDEN = 2 * NEG
LOG2E = 1.4426950408889634
SLOTS = 4
WO_SLOTS = 12
MESH = pl.DeviceIdType.MESH


def _dot(a, b, ca=1, cb=0):
    return lax.dot_general(a, b, (((ca,), (cb,)), ((), ())), preferred_element_type=jnp.float32)


def _kernel(side, x_hbm, gain_ref, cos_ref, sin_ref, wq, wk, wv, wo, y_ref,
            xv, av, wbuf, wobuf, kvs, kvg, qs, qg, os, og, acc, top_s, keep_s, mix_s, s_s,
            x_sem, w_sem, wo_sem, kv_send, kv_recv, g_send, g_recv, q_send, q_recv, o_send, o_recv):
    own, dim = xv.shape
    nc = 4
    nu = nc * CORES
    cols = 2 * HEAD
    group = 2 * cols
    me = lax.axis_index("sp")
    x, y, c = lax.div(me, CORES * side), lax.rem(lax.div(me, CORES), side), lax.rem(me, CORES)
    hx, hy = lax.div(x, 2), lax.div(y, 2)
    gx, gy = lax.rem(x + hx, 2), lax.rem(y + hy, 2)
    u = (hx * 2 + hy) * CORES + c

    def flip(a, d, top=1):
        return a + d * (top - 2 * a)

    def dev(xx, yy, cc):
        return {"sp": (xx * side + yy) * CORES + cc}

    def remote(src, dst, send, recv, to):
        return pltpu.make_async_remote_copy(src_ref=src, dst_ref=dst, send_sem=send, recv_sem=recv, device_id=to, device_id_type=MESH)

    def other(n):
        dx, dy = 1 - lax.rem(n, 2), 1 - lax.div(n, 2)
        return flip(x, dx, side - 1), flip(y, dy, side - 1), flip(hx, dx) * 2 + flip(hy, dy)

    def place(i, fx=0, fy=0):
        ax, ay = flip(gx, fx), flip(gy, fy)
        return flip(ax, lax.div(i, 2), side - 1), flip(ay, lax.rem(i, 2), side - 1)

    def beside(a):
        return a + 1 - 2 * lax.rem(a, 2)

    def load_kv(n):
        _, _, chip = other(jnp.int32(n))
        wide = CORES * HEAD
        at = pl.ds(pl.multiple_of(chip * wide, wide), wide)
        return [pltpu.make_async_copy(wk.at[:, at], wbuf.at[n % SLOTS, :, pl.ds(0, wide)], w_sem.at[n % SLOTS, 0]),
                pltpu.make_async_copy(wv.at[:, at], wbuf.at[n % SLOTS, :, pl.ds(wide, wide)], w_sem.at[n % SLOTS, 1])]

    def target(j):
        xx, yy, chip = other(lax.div(j, CORES))
        cc = flip(c, 1 - lax.rem(j, CORES))
        return xx, yy, cc, chip * CORES + cc

    def load_q(j):
        at = pl.ds(pl.multiple_of(target(j)[3] * group, group), group)
        slot = lax.rem(j + nc, SLOTS)
        return pltpu.make_async_copy(wq.at[:, at], wbuf.at[slot], w_sem.at[slot, 0])

    def load_o(k):
        rows = pl.ds(pl.multiple_of(lax.rem(k, nu) * group + lax.div(k, nu) * cols, cols), cols)
        slot = lax.rem(k, WO_SLOTS)
        return pltpu.make_async_copy(wo.at[rows, :], wobuf.at[slot], wo_sem.at[slot])

    get_x = pltpu.make_async_copy(x_hbm, xv, x_sem)
    get_x.start()
    for copy in load_kv(0):
        copy.start()

    barrier = pltpu.get_barrier_semaphore()
    peers = [dev(flip(x, dx, side - 1), flip(y, dy, side - 1), flip(c, dc)) for dx in range(2) for dy in range(2) for dc in range(2) if dx + dy + dc]
    near = [(beside(x), y), (x, beside(y)), (beside(x), beside(y))]
    peers += [dev(xx, yy, c) for xx, yy in near]
    for peer in peers:
        pl.semaphore_signal(barrier, inc=1, device_id=peer, device_id_type=MESH)

    with jax.named_scope("wait_x"):
        get_x.wait()
    for n in range(1, SLOTS):
        for copy in load_kv(n):
            copy.start()
    wide = xv[...].astype(jnp.float32)
    scale = lax.rsqrt(jnp.mean(wide * wide, -1, keepdims=True) + 1e-6)
    av[...] = (wide * scale * gain_ref[...].astype(jnp.float32)).astype(jnp.bfloat16)
    pl.semaphore_wait(barrier, len(peers))

    def turn(t):
        t = t.astype(jnp.float32)
        return (t * cos_ref[...] + pltpu.roll(t, HEAD // 2, 1) * sin_ref[...]).astype(jnp.bfloat16)

    for n in range(nc):
        with jax.named_scope("wait_wkv"):
            for copy in load_kv(n):
                copy.wait()
        both = _dot(av[...], wbuf[n % SLOTS]).astype(jnp.bfloat16)
        load_q(jnp.int32(n)).start()
        xx, yy, _ = other(jnp.int32(n))
        for h in range(CORES):
            i = n * CORES + h
            kvs[i, :HEAD, :] = turn(both[:, h * HEAD : (h + 1) * HEAD])
            at = (CORES + h) * HEAD
            kvs[i, HEAD:, :] = both[:, at : at + HEAD].T
            there = remote(kvs.at[i], kvg.at[me], kv_send.at[i], kv_recv.at[u], dev(xx, yy, h))
            if n < nc - 1:
                there.start()
            else:
                here = pltpu.make_async_copy(kvs.at[i], kvg.at[me], kv_recv.at[u])
                pl.when(c == h)(here.start)
                pl.when(c != h)(there.start)

    def chip_block(xx, yy):
        return kvg.at[pl.ds((xx * side + yy) * CORES, CORES)]

    def passed(d, i):
        block = chip_block(*place(i))
        return remote(block, block, g_send.at[d, i], g_recv.at[d, i], dev(*near[d], c))

    def arrived(d, i):
        block = chip_block(*place(i, int(d != 1), int(d != 0)))
        return pltpu.make_async_copy(block, block, g_recv.at[d, i])

    def queries(j, _):
        with jax.named_scope("wait_wq"):
            load_q(j).wait()
        slot = lax.rem(j + nc, SLOTS)
        t = _dot(av[...], wbuf[slot]).astype(jnp.bfloat16)

        @pl.when(j + SLOTS < nu)
        def _():
            load_q(j + SLOTS).start()

        @pl.when(j + SLOTS >= nu)
        def _():
            for k in range(2):
                load_o((j + SLOTS - nu) * 2 + k).start()

        for p in range(2):
            for s in range(2):
                at = p * cols + s * HEAD
                qs[j, p, :, s * HEAD : (s + 1) * HEAD] = turn(t[:, at : at + HEAD])
        xx, yy, cc, _ = target(j)
        here = pltpu.make_async_copy(qs.at[j], qg.at[u], q_recv.at[u])
        there = remote(qs.at[j], qg.at[u], q_send.at[j], q_recv.at[u], dev(xx, yy, cc))
        pl.when(j == nu - 1)(here.start)
        pl.when(j < nu - 1)(there.start)

        @pl.when(j < nc)
        def _():
            with jax.named_scope("wait_kvx"):
                for h in range(CORES):
                    pltpu.make_async_copy(kvs.at[0], kvg.at[dev(*place(j), h)["sp"]], kv_recv.at[j * CORES + h]).wait()
            for d in (2, 0, 1):
                passed(d, j).start()

    lax.fori_loop(0, nu, queries, None)
    for k in range(2 * SLOTS, WO_SLOTS):
        load_o(jnp.int32(k)).start()

    e = HEAD**-0.5 * LOG2E
    bk = 2 * CORES * HEAD

    def produce(i, t, chip, p, room):
        k = jnp.concatenate([kvg[t * 2 * CORES + a, :HEAD, :] for a in range(2 * CORES)], axis=0)
        q = qg[chip * CORES + i, p]
        q = jnp.concatenate([q[:, :HEAD], q[:, HEAD:]], axis=0)
        s = _dot(k, q, 1, 1)
        if room is not None:
            gap = lax.rem(lax.broadcasted_iota(jnp.int32, (bk, cols), 1), HEAD) - lax.broadcasted_iota(jnp.int32, (bk, cols), 0)
            s = jnp.where(gap >= -(room + i * HEAD), s, HIDDEN)
        old = top_s[i : i + 1, :]
        top = jnp.maximum(old, s.max(axis=0, keepdims=True))
        top_s[i : i + 1, :] = top
        keep_s[i : i + 1, :] = jnp.exp2((old - top) * e)
        s_s[i] = s

    def consume(i, t):
        v = jnp.concatenate([kvg[t * 2 * CORES + a, HEAD:, :] for a in range(2 * CORES)], axis=1)
        v = jnp.concatenate([v, jnp.ones((8, bk), jnp.bfloat16)], axis=0)
        w = jnp.exp2((s_s[i] - top_s[i : i + 1, :]) * e).astype(jnp.bfloat16)
        mix_s[i] = mix_s[i] * keep_s[i : i + 1, :] + _dot(v, w)

    def item(n, _):
        far, a, b = lax.div(n, 4), lax.rem(lax.div(n, 2), 2), lax.rem(n, 2)
        low, p = a + far * (b - a), b + far * (a - b)
        chip = far * 2 + low
        qx, qy = place(chip)
        index = qx * side + qy
        blocks = lax.div(index, 2) + 1

        @pl.when(lax.rem(n, 4) == 0)
        def _():
            with jax.named_scope("wait_kvg"):
                for d in range(3):
                    for i in range(2):
                        arrived(d, far * 2 + i).wait()

        @pl.when(p == 0)
        def _():
            with jax.named_scope("wait_q"):
                for h in range(CORES):
                    pltpu.make_async_copy(qs.at[0], qg.at[chip * CORES + h], q_recv.at[chip * CORES + h]).wait()

        top_s[...] = jnp.full(top_s.shape, NEG, jnp.float32)
        mix_s[...] = jnp.zeros(mix_s.shape, jnp.float32)
        room = lax.rem(index, 2) * (CORES * HEAD)
        with jax.named_scope("at_first"):
            for i in range(CORES):
                produce(i, 0, chip, p, room + (blocks - 1) * bk)

        def whole(t, _):
            for i in range(CORES):
                consume(i, t - 1)
                produce(i, t, chip, p, None)

        with jax.named_scope("at_whole"):
            lax.fori_loop(1, blocks - 1, whole, None)

        @pl.when(blocks > 1)
        def _():
            for i in range(CORES):
                consume(i, blocks - 2)
                produce(i, blocks - 1, chip, p, room)

        with jax.named_scope("at_last"):
            for i in range(CORES):
                consume(i, blocks - 1)

        for i in range(CORES):
            done = (mix_s[i, :HEAD, :] * (1 / mix_s[i, HEAD : HEAD + 1, :])).astype(jnp.bfloat16)
            for s in range(2):
                os[n, i, :, s * HEAD : (s + 1) * HEAD] = done[:, s * HEAD : (s + 1) * HEAD].T
        for h in range(CORES):
            mine = (chip * CORES + h) == u
            pl.when(mine)(pltpu.make_async_copy(os.at[n, h], og.at[p, u], o_recv.at[p, u]).start)
            pl.when(jnp.logical_not(mine))(sent(n, h, p, qx, qy).start)

    def sent(n, h, p, qx, qy):
        return remote(os.at[n, h], og.at[p, u], o_send.at[n, h], o_recv.at[p, u], dev(qx, qy, h))

    lax.fori_loop(0, nu, item, None)

    step = min(dim, 512)
    for p in range(2):
        with jax.named_scope("wait_o"):
            for k in range(nu):
                pltpu.make_async_copy(os.at[0, 0], og.at[p, k], o_recv.at[p, k]).wait()
        with jax.named_scope("wait_wo"):
            for k in range(nu):
                load_o(jnp.int32(p * nu + k)).wait()

        def columns(n, _):
            at = pl.ds(pl.multiple_of(n * step, step), step)
            more = _dot(og[p, 0], wobuf[(p * nu) % WO_SLOTS, :, at])
            for k in range(1, nu):
                more += _dot(og[p, k], wobuf[(p * nu + k) % WO_SLOTS, :, at])
            if p == 0:
                acc[:, at] = more + xv[:, at].astype(jnp.float32)
            else:
                y_ref[:, at] = (acc[:, at] + more).astype(jnp.bfloat16)

        with jax.named_scope("wo"):
            lax.fori_loop(0, dim // step, columns, None)
        if p == 0:
            for k in range(WO_SLOTS, 2 * nu):
                load_o(jnp.int32(k)).start()

    for n in range(nc):
        xx, yy, _ = other(jnp.int32(n))
        for h in range(CORES):
            i = n * CORES + h
            wait = remote(kvs.at[i], kvg.at[me], kv_send.at[i], kv_recv.at[u], dev(xx, yy, h)).wait_send
            if n < nc - 1:
                wait()
            else:
                pl.when(c != h)(wait)
    for i in range(nc):
        for d in range(3):
            passed(d, jnp.int32(i)).wait_send()

    def left(n, _):
        xx, yy, cc, _ = target(n)
        pl.when(n < nu - 1)(remote(qs.at[n], qg.at[u], q_send.at[n], q_recv.at[u], dev(xx, yy, cc)).wait_send)
        far, a, b = lax.div(n, 4), lax.rem(lax.div(n, 2), 2), lax.rem(n, 2)
        chip, p = far * 2 + a + far * (b - a), b + far * (a - b)
        for h in range(CORES):
            pl.when(chip * CORES + h != u)(sent(n, h, p, *place(chip)).wait_send)

    lax.fori_loop(0, nu, left, None)


def solution(mesh):
    total = mesh.shape["sp"]

    def step(x, gain, wq, wk, wv, wo):
        own, dim = x.shape
        nu = wk.shape[1] // HEAD
        side = math.isqrt(total // CORES)
        group = wq.shape[1] // nu
        place = lax.axis_index("sp") * own + jnp.arange(own)
        half = HEAD // 2
        angle = place.astype(jnp.float32)[:, None] * THETA ** (-jnp.arange(half, dtype=jnp.float32) / half)
        cos, sin = jnp.cos(angle), jnp.sin(angle)
        cos, sin = jnp.concatenate([cos, cos], -1), jnp.concatenate([-sin, sin], -1)
        any_ = pl.BlockSpec(memory_space=pltpu.HBM)
        vmem = pl.BlockSpec(memory_space=pltpu.VMEM)
        low, wide = jnp.bfloat16, jnp.float32
        dma = pltpu.SemaphoreType.DMA
        cols = 2 * HEAD
        return pl.pallas_call(
            functools.partial(_kernel, side),
            out_shape=jax.ShapeDtypeStruct((own, dim), low),
            in_specs=[any_, vmem, vmem, vmem, any_, any_, any_, any_],
            out_specs=vmem,
            scratch_shapes=[
                pltpu.VMEM((own, dim), low),
                pltpu.VMEM((own, dim), low),
                pltpu.VMEM((SLOTS, dim, group), low),
                pltpu.VMEM((WO_SLOTS, cols, dim), low),
                pltpu.VMEM((nu, 2 * HEAD, own), low),
                pltpu.VMEM((total, 2 * HEAD, own), low),
                pltpu.VMEM((nu, 2, own, cols), low),
                pltpu.VMEM((nu, 2, own, cols), low),
                pltpu.VMEM((nu, CORES, own, cols), low),
                pltpu.VMEM((2, nu, own, cols), low),
                pltpu.VMEM((own, dim), wide),
                pltpu.VMEM((CORES, cols), wide),
                pltpu.VMEM((CORES, cols), wide),
                pltpu.VMEM((CORES, HEAD + 8, cols), wide),
                pltpu.VMEM((CORES, 2 * CORES * HEAD, cols), wide),
                dma, dma((SLOTS, 2)), dma((WO_SLOTS,)),
                dma((nu,)), dma((nu,)), dma((3, 4)), dma((3, 4)),
                dma((nu,)), dma((nu,)), dma((nu, CORES)), dma((2, nu)),
            ],
            compiler_params=pltpu.CompilerParams(collective_id=0, has_side_effects=True, vmem_limit_bytes=63 * 2**20),
        )(x, gain[None], cos, sin, wq, wk, wv, wo)

    tokens, whole = P(("dp", "sp"), None), P(None, None)
    return jax.shard_map(
        step,
        mesh=mesh,
        in_specs=(tokens, P(None), whole, whole, whole, whole),
        out_specs=tokens,
        check_vma=False,
    )
```

```python
import functools
import math

import jax
import jax.numpy as jnp
from jax import lax
from jax.experimental import pallas as pl
from jax.experimental.pallas import tpu as pltpu
from jax.sharding import PartitionSpec as P

HEAD = 128
THETA = 10000
CORES = 2
NEG = -1e30
HIDDEN = 2 * NEG
LOG2E = 1.4426950408889634
SLOTS = 3
MESH = pl.DeviceIdType.MESH
PASSES = [[(0, 0)], [(0, 1)], [], [], [(1, 0), (1, 1)], [(0, 2)], [(0, 3)], []]


def _dot(a, b, ca=1, cb=0):
    return lax.dot_general(a, b, (((ca,), (cb,)), ((), ())), preferred_element_type=jnp.float32)


def _kernel(side, x_hbm, gain_ref, cos_ref, sin_ref, wq, wk, wv, wo, y_ref,
            xv, av, wbuf, wobuf, kvs, kvg, qs, qg, os, og, acc, top_s, keep_s, mix_s, s_s,
            x_sem, w_sem, wo_sem, kv_send, kv_recv, g_send, g_recv, q_send, q_recv, o_send, o_recv):
    own, dim = xv.shape
    nc = 4
    nu = nc * CORES
    cols = 2 * HEAD
    group = 2 * cols
    me = lax.axis_index("sp")
    x, y, c = lax.div(me, CORES * side), lax.rem(lax.div(me, CORES), side), lax.rem(me, CORES)
    hx, hy = lax.div(x, 2), lax.div(y, 2)
    gx, gy = lax.rem(x + hx, 2), lax.rem(y + hy, 2)
    u = (hx * 2 + hy) * CORES + c

    def flip(a, d, top=1):
        return a + d * (top - 2 * a)

    def dev(xx, yy, cc):
        return {"sp": (xx * side + yy) * CORES + cc}

    def remote(src, dst, send, recv, to):
        return pltpu.make_async_remote_copy(src_ref=src, dst_ref=dst, send_sem=send, recv_sem=recv, device_id=to, device_id_type=MESH)

    def other(n):
        dx, dy = 1 - lax.rem(n, 2), 1 - lax.div(n, 2)
        return flip(x, dx, side - 1), flip(y, dy, side - 1), flip(hx, dx) * 2 + flip(hy, dy)

    def place(i, fx=0, fy=0):
        ax, ay = flip(gx, fx), flip(gy, fy)
        return flip(ax, i // 2, side - 1), flip(ay, i % 2, side - 1)

    def beside(a):
        return a + 1 - 2 * lax.rem(a, 2)

    def load_kv(n):
        _, _, chip = other(jnp.int32(n))
        wide = CORES * HEAD
        at = pl.ds(pl.multiple_of(chip * wide, wide), wide)
        return [pltpu.make_async_copy(wk.at[:, at], wbuf.at[n % SLOTS, :, pl.ds(0, wide)], w_sem.at[n % SLOTS, 0]),
                pltpu.make_async_copy(wv.at[:, at], wbuf.at[n % SLOTS, :, pl.ds(wide, wide)], w_sem.at[n % SLOTS, 1])]

    def target(j):
        xx, yy, chip = other(lax.div(j, CORES))
        cc = flip(c, 1 - lax.rem(j, CORES))
        return xx, yy, cc, chip * CORES + cc

    def load_q(j):
        at = pl.ds(pl.multiple_of(target(j)[3] * group, group), group)
        slot = lax.rem(j + nc, SLOTS)
        return pltpu.make_async_copy(wq.at[:, at], wbuf.at[slot], w_sem.at[slot, 0])

    step = wobuf.shape[3]
    slabs = dim // step

    def load_o(p, n):
        at = pl.ds(pl.multiple_of(n * step, step), step)
        return pltpu.make_async_copy(wo.at[:, p, :, at], wobuf.at[p * slabs + n], wo_sem.at[p * slabs + n])

    get_x = pltpu.make_async_copy(x_hbm, xv, x_sem)
    get_x.start()
    for copy in load_kv(0):
        copy.start()

    barrier = pltpu.get_barrier_semaphore()
    peers = [dev(flip(x, dx, side - 1), flip(y, dy, side - 1), flip(c, dc)) for dx in range(2) for dy in range(2) for dc in range(2) if dx + dy + dc]
    near = [(beside(x), y), (x, beside(y))]
    peers += [dev(xx, yy, c) for xx, yy in near]
    for peer in peers:
        pl.semaphore_signal(barrier, inc=1, device_id=peer, device_id_type=MESH)

    with jax.named_scope("wait_x"):
        get_x.wait()
    for n in range(1, SLOTS):
        for copy in load_kv(n):
            copy.start()
    wide = xv[...].astype(jnp.float32)
    scale = lax.rsqrt(jnp.mean(wide * wide, -1, keepdims=True) + 1e-6)
    av[...] = (wide * scale * gain_ref[...].astype(jnp.float32)).astype(jnp.bfloat16)
    pl.semaphore_wait(barrier, len(peers))

    def turn(t):
        t = t.astype(jnp.float32)
        return (t * cos_ref[...] + pltpu.roll(t, HEAD // 2, 1) * sin_ref[...]).astype(jnp.bfloat16)

    for n in range(nc):
        with jax.named_scope("wait_wkv"):
            for copy in load_kv(n):
                copy.wait()
        both = _dot(av[...], wbuf[n % SLOTS]).astype(jnp.bfloat16)
        if n + SLOTS < nc:
            for copy in load_kv(n + SLOTS):
                copy.start()
        else:
            load_q(jnp.int32(n + SLOTS - nc)).start()
        xx, yy, _ = other(jnp.int32(n))
        for h in range(CORES):
            i = n * CORES + h
            kvs[i, :HEAD, :] = turn(both[:, h * HEAD : (h + 1) * HEAD])
            at = (CORES + h) * HEAD
            kvs[i, HEAD:, :] = both[:, at : at + HEAD].T
            there = remote(kvs.at[i], kvg.at[me], kv_send.at[i], kv_recv.at[u], dev(xx, yy, h))
            if n < nc - 1:
                there.start()
            else:
                here = pltpu.make_async_copy(kvs.at[i], kvg.at[me], kv_recv.at[u])
                pl.when(c == h)(here.start)
                pl.when(c != h)(there.start)

    def chip_block(xx, yy):
        return kvg.at[pl.ds((xx * side + yy) * CORES, CORES)]

    def passed(d, i):
        block = chip_block(*place(i))
        return remote(block, block, g_send.at[d, i], g_recv.at[d, i], dev(*near[d], c))

    def relayed(i):
        block = chip_block(*place(i, i % 2, 1 - i % 2))
        return remote(block, block, g_send.at[2, i], g_recv.at[2, i], dev(*near[i % 2], c))

    def arrived(d, i):
        with jax.named_scope("wait_kvg"):
            block = chip_block(*place(i, int(d != 1), int(d != 0)))
            pltpu.make_async_copy(block, block, g_recv.at[d, i]).wait()

    def relay(i):
        arrived(1 - i % 2, i)
        relayed(i).start()

    def pass_on(i):
        with jax.named_scope("wait_kvx"):
            for h in range(CORES):
                pltpu.make_async_copy(kvs.at[0], kvg.at[dev(*place(i), h)["sp"]], kv_recv.at[i * CORES + h]).wait()
        for d in range(2):
            passed(d, i).start()

    def queries(j, _):
        with jax.named_scope("wait_wq"):
            load_q(j).wait()
        slot = lax.rem(j + nc, SLOTS)
        t = _dot(av[...], wbuf[slot]).astype(jnp.bfloat16)

        @pl.when(j + SLOTS < nu)
        def _():
            load_q(j + SLOTS).start()

        @pl.when(j + SLOTS >= nu)
        def _():
            load_o(0, j + SLOTS - nu).start()

        for p in range(2):
            for s in range(2):
                at = p * cols + s * HEAD
                qs[j, p, :, s * HEAD : (s + 1) * HEAD] = turn(t[:, at : at + HEAD])
        xx, yy, cc, _ = target(j)
        here = pltpu.make_async_copy(qs.at[j], qg.at[u], q_recv.at[u])
        there = remote(qs.at[j], qg.at[u], q_send.at[j], q_recv.at[u], dev(xx, yy, cc))
        pl.when(j == nu - 1)(here.start)
        pl.when(j < nu - 1)(there.start)

        for at, do in enumerate(PASSES):
            for f, i in do:
                pl.when(j == at)(functools.partial((pass_on, relay)[f], i))

    lax.fori_loop(0, nu, queries, None)
    for n in range(SLOTS, slabs):
        load_o(0, n).start()
    for n in range(slabs):
        load_o(1, n).start()

    e = HEAD**-0.5 * LOG2E
    row = side * CORES
    bk = row * HEAD

    def of(n):
        far, a, b = lax.div(n, 4), lax.rem(lax.div(n, 2), 2), lax.rem(n, 2)
        return far * 2 + a + far * (b - a), b + far * (a - b)

    def produce(i, n, t, room):
        chip, p = of(n)
        k = jnp.concatenate([kvg[t * row + a, :HEAD, :] for a in range(row)], axis=0)
        q = qg[chip * CORES + i, p]
        q = jnp.concatenate([q[:, :HEAD], q[:, HEAD:]], axis=0)
        s = _dot(k, q, 1, 1)
        if room is not None:
            gap = lax.rem(lax.broadcasted_iota(jnp.int32, (bk, cols), 1), HEAD) - lax.broadcasted_iota(jnp.int32, (bk, cols), 0)
            s = jnp.where(gap >= -(room + i * HEAD), s, HIDDEN)
        old = top_s[n, i : i + 1, :]
        top = jnp.maximum(old, s.max(axis=0, keepdims=True))
        top_s[n, i : i + 1, :] = top
        keep_s[n, i : i + 1, :] = jnp.exp2((old - top) * e)
        s_s[i] = s

    def consume(i, n, t):
        v = jnp.concatenate([kvg[t * row + a, HEAD:, :] for a in range(row)], axis=1)
        v = jnp.concatenate([v, jnp.ones((8, bk), jnp.bfloat16)], axis=0)
        w = jnp.exp2((s_s[i] - top_s[n, i : i + 1, :]) * e).astype(jnp.bfloat16)
        mix_s[n, i] = mix_s[n, i] * keep_s[n, i : i + 1, :] + _dot(v, w)

    def last(n):
        return gx + lax.div(n, 4) * (side - 1 - 2 * gx)

    def room(n, t):
        chip, _ = of(n)
        qx, qy = place(chip)
        return (qx - t) * bk + qy * (CORES * HEAD)

    def both(n, t, m, s, masked):
        for i in range(CORES):
            consume(i, m, s)
            produce(i, n, t, room(n, t) if masked else None)

    def sent(n, h, p, qx, qy):
        return remote(os.at[n, h], og.at[p, u], o_send.at[n, h], o_recv.at[p, u], dev(qx, qy, h))

    def finish(n):
        chip, p = of(n)
        qx, qy = place(chip)
        for i in range(CORES):
            done = (mix_s[n, i, :HEAD, :] * (1 / mix_s[n, i, HEAD : HEAD + 1, :])).astype(jnp.bfloat16)
            for s in range(2):
                os[n, i, :, s * HEAD : (s + 1) * HEAD] = done[:, s * HEAD : (s + 1) * HEAD].T
        for h in range(CORES):
            mine = (chip * CORES + h) == u
            pl.when(mine)(pltpu.make_async_copy(os.at[n, h], og.at[p, u], o_recv.at[p, u]).start)
            pl.when(jnp.logical_not(mine))(sent(n, h, p, qx, qy).start)

    def take_q(n, t):
        chip, p = of(n)

        @pl.when(t + p == 0)
        def _():
            with jax.named_scope("wait_q"):
                for h in range(CORES):
                    pltpu.make_async_copy(qs.at[0], qg.at[chip * CORES + h], q_recv.at[chip * CORES + h]).wait()

    def advance(n, t, m, s):
        take_q(n, t)
        pl.when(t == last(n))(lambda: both(n, t, m, s, True))
        pl.when(t < last(n))(lambda: both(n, t, m, s, False))
        pl.when(s == last(m))(lambda: finish(m))
        return n, t

    top_s[...] = jnp.full(top_s.shape, NEG, jnp.float32)
    mix_s[...] = jnp.zeros(mix_s.shape, jnp.float32)

    def early():
        for d, i in ((0, 0), (2, 0), (2, 1)):
            arrived(d, i)

    arrived(1, 1)
    pl.when(gx == 1)(early)
    zero = jnp.int32(0)
    take_q(zero, zero)
    for i in range(CORES):
        produce(i, zero, zero, room(zero, zero))

    def first_steps(g, before):
        pl.when(g == 3)(lambda: relay(2))
        with jax.named_scope("near"):
            return advance((1 - gx) * g + gx * lax.div(g, 2), gx * lax.rem(g, 2), *before)

    at = lax.fori_loop(1, 4 * (gx + 1), first_steps, (zero, zero))
    pl.when(gx == 0)(early)

    def middle_steps(g, before):
        pl.when(g == 1)(lambda: relay(3))
        n, t = 4 + lax.div(g, 2), lax.rem(g, 2)
        take_q(n, t)
        m, s = before
        with jax.named_scope("mid"):
            both(n, t, m, s, False)
        pl.when((g == 0) & (s == last(m)))(lambda: finish(m))
        return n, t

    at = lax.fori_loop(0, 8, middle_steps, at)
    for d, i in ((0, 2), (1, 3), (2, 2), (2, 3)):
        arrived(d, i)

    def late_steps(g, before):
        with jax.named_scope("far"):
            return advance(4 + gx * g + (1 - gx) * lax.div(g, 2), 2 + (1 - gx) * lax.rem(g, 2), *before)

    at = lax.fori_loop(0, 4 * (2 - gx), late_steps, at)
    for i in range(CORES):
        consume(i, *at)
    finish(at[0])

    for p in range(2):
        with jax.named_scope("wait_o"):
            for k in range(nu):
                pltpu.make_async_copy(os.at[0, 0], og.at[p, k], o_recv.at[p, k]).wait()

        def columns(n, _):
            at = pl.ds(pl.multiple_of(n * step, step), step)
            load_o(p, n).wait()
            more = _dot(og[p, 0], wobuf[p * slabs + n, 0])
            for k in range(1, nu):
                more += _dot(og[p, k], wobuf[p * slabs + n, k])
            if p == 0:
                acc[:, at] = more + xv[:, at].astype(jnp.float32)
            else:
                y_ref[:, at] = (acc[:, at] + more).astype(jnp.bfloat16)

        with jax.named_scope("wo"):
            lax.fori_loop(0, slabs, columns, None)

    for n in range(nc):
        xx, yy, _ = other(jnp.int32(n))
        for h in range(CORES):
            i = n * CORES + h
            wait = remote(kvs.at[i], kvg.at[me], kv_send.at[i], kv_recv.at[u], dev(xx, yy, h)).wait_send
            if n < nc - 1:
                wait()
            else:
                pl.when(c != h)(wait)
    for i in range(nc):
        for d in range(2):
            passed(d, i).wait_send()
        relayed(i).wait_send()

    def left(n, _):
        xx, yy, cc, _ = target(n)
        pl.when(n < nu - 1)(remote(qs.at[n], qg.at[u], q_send.at[n], q_recv.at[u], dev(xx, yy, cc)).wait_send)
        chip, p = of(n)
        for h in range(CORES):
            pl.when(chip * CORES + h != u)(sent(n, h, p, *place(chip)).wait_send)

    lax.fori_loop(0, nu, left, None)


def solution(mesh):
    total = mesh.shape["sp"]

    def step(x, gain, wq, wk, wv, wo):
        own, dim = x.shape
        nu = wk.shape[1] // HEAD
        side = math.isqrt(total // CORES)
        group = wq.shape[1] // nu
        place = lax.axis_index("sp") * own + jnp.arange(own)
        half = HEAD // 2
        angle = place.astype(jnp.float32)[:, None] * THETA ** (-jnp.arange(half, dtype=jnp.float32) / half)
        cos, sin = jnp.cos(angle), jnp.sin(angle)
        cos, sin = jnp.concatenate([cos, cos], -1), jnp.concatenate([-sin, sin], -1)
        any_ = pl.BlockSpec(memory_space=pltpu.HBM)
        vmem = pl.BlockSpec(memory_space=pltpu.VMEM)
        low, wide = jnp.bfloat16, jnp.float32
        dma = pltpu.SemaphoreType.DMA
        cols = 2 * HEAD
        step_o = min(dim, 512)
        return pl.pallas_call(
            functools.partial(_kernel, side),
            out_shape=jax.ShapeDtypeStruct((own, dim), low),
            in_specs=[any_, vmem, vmem, vmem, any_, any_, any_, any_],
            out_specs=vmem,
            scratch_shapes=[
                pltpu.VMEM((own, dim), low),
                pltpu.VMEM((own, dim), low),
                pltpu.VMEM((SLOTS, dim, group), low),
                pltpu.VMEM((2 * dim // step_o, nu, cols, step_o), low),
                pltpu.VMEM((nu, 2 * HEAD, own), low),
                pltpu.VMEM((total, 2 * HEAD, own), low),
                pltpu.VMEM((nu, 2, own, cols), low),
                pltpu.VMEM((nu, 2, own, cols), low),
                pltpu.VMEM((nu, CORES, own, cols), low),
                pltpu.VMEM((2, nu, own, cols), low),
                pltpu.VMEM((own, dim), wide),
                pltpu.VMEM((nu, CORES, cols), wide),
                pltpu.VMEM((nu, CORES, cols), wide),
                pltpu.VMEM((nu, CORES, HEAD + 8, cols), wide),
                pltpu.VMEM((CORES, side * CORES * own, cols), wide),
                dma, dma((SLOTS, 2)), dma((2 * dim // step_o,)),
                dma((nu,)), dma((nu,)), dma((3, 4)), dma((3, 4)),
                dma((nu,)), dma((nu,)), dma((nu, CORES)), dma((2, nu)),
            ],
            compiler_params=pltpu.CompilerParams(collective_id=0, has_side_effects=True, vmem_limit_bytes=63 * 2**20),
        )(x, gain[None], cos, sin, wq, wk, wv, wo.reshape(nu, 2, cols, dim))

    tokens, whole = P(("dp", "sp"), None), P(None, None)
    return jax.shard_map(
        step,
        mesh=mesh,
        in_specs=(tokens, P(None), whole, whole, whole, whole),
        out_specs=tokens,
        check_vma=False,
    )
```

```python
import functools
import math

import jax
import jax.numpy as jnp
from jax import lax
from jax.experimental import pallas as pl
from jax.experimental.pallas import tpu as pltpu
from jax.sharding import PartitionSpec as P

HEAD = 128
THETA = 10000
CORES = 2
NEG = -1e30
HIDDEN = 2 * NEG
LOG2E = 1.4426950408889634
SLOTS = 3
MESH = pl.DeviceIdType.MESH
PASSES = [[(0, 0)], [(0, 1)], [(0, 2)], [], [], [], [], [(1, 0)]]


def _dot(a, b, ca=1, cb=0):
    return lax.dot_general(a, b, (((ca,), (cb,)), ((), ())), preferred_element_type=jnp.float32)


def _kernel(side, x_hbm, gain_ref, rate_ref, wq, wk, wv, wo, y_hbm,
            xv, av, cos_ref, sin_ref, wbuf, wobuf, kvs, kvg, qs, qg, os, og, acc, top_s, keep_s, mix_s, s_s,
            x_sem, w_sem, wo_sem, kv_send, kv_recv, g_send, g_recv, q_send, q_recv, o_send, o_recv):
    own, dim = xv.shape
    nc = 4
    nu = nc * CORES
    cols = 2 * HEAD
    group = 2 * cols
    me = lax.axis_index("sp")
    x, y, c = lax.div(me, CORES * side), lax.rem(lax.div(me, CORES), side), lax.rem(me, CORES)
    hx, hy = lax.div(x, 2), lax.div(y, 2)
    gx, gy = lax.rem(x + hx, 2), lax.rem(y + hy, 2)
    u = (hx * 2 + hy) * CORES + c

    def flip(a, d, top=1):
        return a + d * (top - 2 * a)

    def dev(xx, yy, cc):
        return {"sp": (xx * side + yy) * CORES + cc}

    def remote(src, dst, send, recv, to):
        return pltpu.make_async_remote_copy(src_ref=src, dst_ref=dst, send_sem=send, recv_sem=recv, device_id=to, device_id_type=MESH)

    def other(n):
        dx, dy = 1 - lax.rem(n, 2), 1 - lax.div(n, 2)
        return flip(x, dx, side - 1), flip(y, dy, side - 1), flip(hx, dx) * 2 + flip(hy, dy)

    def place(i, fx=0, fy=0):
        ax, ay = flip(gx, fx), flip(gy, fy)
        return flip(ax, i // 2, side - 1), flip(ay, i % 2, side - 1)

    def beside(a):
        return a + 1 - 2 * lax.rem(a, 2)

    def load_kv(n):
        _, _, chip = other(jnp.int32(n))
        wide = CORES * HEAD
        at = pl.ds(pl.multiple_of(chip * wide, wide), wide)
        return [pltpu.make_async_copy(wk.at[:, at], wbuf.at[n % SLOTS, :, pl.ds(0, wide)], w_sem.at[n % SLOTS, 0]),
                pltpu.make_async_copy(wv.at[:, at], wbuf.at[n % SLOTS, :, pl.ds(wide, wide)], w_sem.at[n % SLOTS, 1])]

    def target(j):
        xx, yy, chip = other(lax.div(j, CORES))
        cc = flip(c, 1 - lax.rem(j, CORES))
        return xx, yy, cc, chip * CORES + cc

    def load_q(j):
        at = pl.ds(pl.multiple_of(target(j)[3] * group, group), group)
        slot = lax.rem(j + nc, SLOTS)
        return pltpu.make_async_copy(wq.at[:, at], wbuf.at[slot], w_sem.at[slot, 0])

    step = wobuf.shape[3]
    slabs = dim // step

    def load_o(p, n):
        at = pl.ds(pl.multiple_of(n * step, step), step)
        return pltpu.make_async_copy(wo.at[:, p, :, at], wobuf.at[p * slabs + n], wo_sem.at[p * slabs + n])

    get_x = pltpu.make_async_copy(x_hbm, xv, x_sem)
    get_x.start()
    for copy in load_kv(0):
        copy.start()

    barrier = pltpu.get_barrier_semaphore()
    peers = [dev(flip(x, dx, side - 1), flip(y, dy, side - 1), flip(c, dc)) for dx in range(2) for dy in range(2) for dc in range(2) if dx + dy + dc]
    near = [(beside(x), y), (x, beside(y))]
    peers += [dev(xx, yy, c) for xx, yy in near]
    for peer in peers:
        pl.semaphore_signal(barrier, inc=1, device_id=peer, device_id_type=MESH)

    place_ = (me * own + lax.broadcasted_iota(jnp.int32, (own, HEAD), 0)).astype(jnp.float32)
    angle = place_ * rate_ref[...]
    second = lax.broadcasted_iota(jnp.int32, (own, HEAD), 1) >= HEAD // 2
    cos_ref[...] = jnp.cos(angle)
    sin_ref[...] = jnp.where(second, jnp.sin(angle), -jnp.sin(angle))
    with jax.named_scope("wait_x"):
        get_x.wait()
    for n in range(1, SLOTS):
        for copy in load_kv(n):
            copy.start()
    wide = xv[...].astype(jnp.float32)
    scale = lax.rsqrt(jnp.mean(wide * wide, -1, keepdims=True) + 1e-6)
    lanes = gain_ref.shape[1]
    for k in range(dim // lanes):
        at = slice(k * lanes, (k + 1) * lanes)
        av[:, at] = (xv[:, at].astype(jnp.float32) * scale * gain_ref[k : k + 1, :].astype(jnp.float32)).astype(jnp.bfloat16)
    with jax.named_scope("wait_b"):
        pl.semaphore_wait(barrier, len(peers))

    def turn(t):
        t = t.astype(jnp.float32)
        return (t * cos_ref[...] + pltpu.roll(t, HEAD // 2, 1) * sin_ref[...]).astype(jnp.bfloat16)

    for n in range(nc):
        with jax.named_scope("wait_wkv"):
            for copy in load_kv(n):
                copy.wait()
        both = _dot(av[...], wbuf[n % SLOTS]).astype(jnp.bfloat16)
        if n + SLOTS < nc:
            for copy in load_kv(n + SLOTS):
                copy.start()
        else:
            load_q(jnp.int32(n + SLOTS - nc)).start()
        xx, yy, _ = other(jnp.int32(n))
        for h in range(CORES):
            i = n * CORES + h
            kvs[i, :HEAD, :] = turn(both[:, h * HEAD : (h + 1) * HEAD])
            at = (CORES + h) * HEAD
            kvs[i, HEAD:, :] = both[:, at : at + HEAD].T
            there = remote(kvs.at[i], kvg.at[me], kv_send.at[i], kv_recv.at[u], dev(xx, yy, h))
            if n < nc - 1:
                there.start()
            else:
                here = pltpu.make_async_copy(kvs.at[i], kvg.at[me], kv_recv.at[u])
                pl.when(c == h)(here.start)
                pl.when(c != h)(there.start)

    def chip_block(xx, yy):
        return kvg.at[pl.ds((xx * side + yy) * CORES, CORES)]

    def passed(d, i):
        block = chip_block(*place(i))
        return remote(block, block, g_send.at[d, i], g_recv.at[d, i], dev(*near[d], c))

    def relayed(i):
        block = chip_block(*place(i, i % 2, 1 - i % 2))
        return remote(block, block, g_send.at[2, i], g_recv.at[2, i], dev(*near[i % 2], c))

    def arrived(d, i):
        with jax.named_scope("wait_kvg"):
            block = chip_block(*place(i, int(d != 1), int(d != 0)))
            pltpu.make_async_copy(block, block, g_recv.at[d, i]).wait()

    def relay(i):
        arrived(1 - i % 2, i)
        relayed(i).start()

    def pass_on(i):
        with jax.named_scope("wait_kvx"):
            for h in range(CORES):
                pltpu.make_async_copy(kvs.at[0], kvg.at[dev(*place(i), h)["sp"]], kv_recv.at[i * CORES + h]).wait()
        for d in range(2):
            passed(d, i).start()

    def queries(j, _):
        with jax.named_scope("wait_wq"):
            load_q(j).wait()
        slot = lax.rem(j + nc, SLOTS)
        t = _dot(av[...], wbuf[slot]).astype(jnp.bfloat16)

        @pl.when(j + SLOTS < nu)
        def _():
            load_q(j + SLOTS).start()

        @pl.when(j + SLOTS >= nu)
        def _():
            load_o(0, j + SLOTS - nu).start()

        for p in range(2):
            for s in range(2):
                at = p * cols + s * HEAD
                qs[j, p, :, s * HEAD : (s + 1) * HEAD] = turn(t[:, at : at + HEAD])
        xx, yy, cc, _ = target(j)
        here = pltpu.make_async_copy(qs.at[j], qg.at[u], q_recv.at[u])
        there = remote(qs.at[j], qg.at[u], q_send.at[j], q_recv.at[u], dev(xx, yy, cc))
        pl.when(j == nu - 1)(here.start)
        pl.when(j < nu - 1)(there.start)

        for at, do in enumerate(PASSES):
            for f, i in do:
                pl.when(j == at)(functools.partial((pass_on, relay)[f], i))

    lax.fori_loop(0, nu, queries, None)
    for n in range(SLOTS, slabs):
        load_o(0, n).start()
    for n in range(slabs):
        load_o(1, n).start()

    e = HEAD**-0.5 * LOG2E
    row = side * CORES
    bk = row * HEAD

    def of(n):
        return lax.div(n, 4) * 2 + lax.rem(n, 2), lax.rem(lax.div(n, 2), 2)

    def produce(i, n, t, room):
        chip, p = of(n)
        k = jnp.concatenate([kvg[t * row + a, :HEAD, :] for a in range(row)], axis=0)
        q = qg[chip * CORES + i, p]
        q = jnp.concatenate([q[:, :HEAD], q[:, HEAD:]], axis=0)
        s = _dot(k, q, 1, 1)
        if room is not None:
            gap = lax.rem(lax.broadcasted_iota(jnp.int32, (bk, cols), 1), HEAD) - lax.broadcasted_iota(jnp.int32, (bk, cols), 0)
            s = jnp.where(gap >= -(room + i * HEAD), s, HIDDEN)
        old = top_s[n, i : i + 1, :]
        top = jnp.maximum(old, s.max(axis=0, keepdims=True))
        top_s[n, i : i + 1, :] = top
        keep_s[n, i : i + 1, :] = jnp.exp2((old - top) * e)
        s_s[i] = s

    def consume(i, n, t):
        v = jnp.concatenate([kvg[t * row + a, HEAD:, :] for a in range(row)], axis=1)
        v = jnp.concatenate([v, jnp.ones((8, bk), jnp.bfloat16)], axis=0)
        w = jnp.exp2((s_s[i] - top_s[n, i : i + 1, :]) * e).astype(jnp.bfloat16)
        mix_s[n, i] = mix_s[n, i] * keep_s[n, i : i + 1, :] + _dot(v, w)

    def both(n, t, m, s, masked):
        for i in range(CORES):
            consume(i, m, s)
        room = place(of(n)[0])[1] * (CORES * HEAD) if masked else None
        for i in range(CORES):
            produce(i, n, t, room)

    def sent(n, h, p, qx, qy):
        return remote(os.at[n, h], og.at[p, u], o_send.at[n, h], o_recv.at[p, u], dev(qx, qy, h))

    def finish(n):
        chip, p = of(n)
        qx, qy = place(chip)
        for i in range(CORES):
            done = (mix_s[n, i, :HEAD, :] * (1 / mix_s[n, i, HEAD : HEAD + 1, :])).astype(jnp.bfloat16)
            for s in range(2):
                os[n, i, :, s * HEAD : (s + 1) * HEAD] = done[:, s * HEAD : (s + 1) * HEAD].T
        for h in range(CORES):
            mine = (chip * CORES + h) == u
            pl.when(mine)(pltpu.make_async_copy(os.at[n, h], og.at[p, u], o_recv.at[p, u]).start)
            pl.when(jnp.logical_not(mine))(sent(n, h, p, qx, qy).start)

    def take_q(n):
        chip, p = of(n)

        @pl.when(p == 0)
        def _():
            with jax.named_scope("wait_q"):
                for h in range(CORES):
                    pltpu.make_async_copy(qs.at[0], qg.at[chip * CORES + h], q_recv.at[chip * CORES + h]).wait()

    top_s[...] = jnp.full(top_s.shape, NEG, jnp.float32)
    mix_s[...] = jnp.zeros(mix_s.shape, jnp.float32)

    arrived(1, 1)
    zero = jnp.int32(0)
    take_q(zero)
    for i in range(CORES):
        produce(i, zero, gx, gy * (CORES * HEAD))

    def early_own(n, _):
        @pl.when(n == 1)
        def _():
            relay(1)
            pass_on(3)

        take_q(n)
        with jax.named_scope("p1"):
            both(n, gx, n - 1, gx, True)
        pl.when(gx == 0)(lambda: finish(n - 1))

    lax.fori_loop(1, 4, early_own, None)

    def late_first(g, before):
        pl.when(g == 1)(lambda: relay(2))

        @pl.when(g == 4)
        def _():
            for d, i in ((0, 0), (2, 0), (2, 1)):
                arrived(d, i)

        pl.when(g == 6)(lambda: relay(3))
        n, t = 4 + lax.rem(g, 4), gx + lax.div(g, 4) * (1 - 2 * gx)
        pl.when(g < 4)(lambda: take_q(n))
        with jax.named_scope("p2"):
            both(n, t, *before, False)
        pl.when((g == 0) & (gx == 0))(lambda: finish(jnp.int32(3)))
        return n, t

    at = lax.fori_loop(0, 8, late_first, (jnp.int32(3), gx))
    arrived(1, 3)

    def late_own(g, before):
        n, t = 4 + g, side - 1 - gx
        with jax.named_scope("p3"):
            both(n, t, *before, True)
        pl.when((g > 0) & (gx == 1))(lambda: finish(before[0]))
        return n, t

    at = lax.fori_loop(0, 4, late_own, at)

    def last_gather():
        for d, i in ((0, 2), (2, 2), (2, 3)):
            arrived(d, i)

    pl.when(gx == 0)(last_gather)

    def rest(g, before):
        n, t = g + 4 * (1 - gx), 2 * (1 - gx)
        with jax.named_scope("p4"):
            both(n, t, *before, False)
        pl.when(g + gx > 0)(lambda: finish(before[0]))
        return n, t

    at = lax.fori_loop(0, 4, rest, at)
    for i in range(CORES):
        consume(i, *at)
    finish(at[0])

    for p in range(2):
        with jax.named_scope("wait_o"):
            for k in range(nu):
                pltpu.make_async_copy(os.at[0, 0], og.at[p, k], o_recv.at[p, k]).wait()

        with jax.named_scope("wait_wo"):
            for n in range(slabs):
                load_o(p, n).wait()
        with jax.named_scope("wo"):
            for n in range(slabs):
                more = _dot(og[p, 0], wobuf[p * slabs + n, 0])
                for k in range(1, nu):
                    more += _dot(og[p, k], wobuf[p * slabs + n, k])
                if p == 0:
                    acc[:, n * step : (n + 1) * step] = more
                else:
                    acc[:, n * step : (n + 1) * step] += more
    put = pltpu.make_async_copy(acc, y_hbm, x_sem)
    put.start()

    for n in range(nc):
        xx, yy, _ = other(jnp.int32(n))
        for h in range(CORES):
            i = n * CORES + h
            wait = remote(kvs.at[i], kvg.at[me], kv_send.at[i], kv_recv.at[u], dev(xx, yy, h)).wait_send
            if n < nc - 1:
                wait()
            else:
                pl.when(c != h)(wait)
    for i in range(nc):
        for d in range(2):
            passed(d, i).wait_send()
        relayed(i).wait_send()

    def left(n, _):
        xx, yy, cc, _ = target(n)
        pl.when(n < nu - 1)(remote(qs.at[n], qg.at[u], q_send.at[n], q_recv.at[u], dev(xx, yy, cc)).wait_send)
        chip, p = of(n)
        for h in range(CORES):
            pl.when(chip * CORES + h != u)(sent(n, h, p, *place(chip)).wait_send)

    lax.fori_loop(0, nu, left, None)
    pl.when(gx == 1)(last_gather)
    put.wait()


def solution(mesh):
    total = mesh.shape["sp"]

    def step(x, gain, wq, wk, wv, wo):
        own, dim = x.shape
        nu = wk.shape[1] // HEAD
        side = math.isqrt(total // CORES)
        group = wq.shape[1] // nu
        half = HEAD // 2
        rate = THETA ** (-jnp.arange(half, dtype=jnp.float32) / half)
        rate = jnp.concatenate([rate, rate])[None]
        any_ = pl.BlockSpec(memory_space=pltpu.HBM)
        vmem = pl.BlockSpec(memory_space=pltpu.VMEM)
        low, wide = jnp.bfloat16, jnp.float32
        dma = pltpu.SemaphoreType.DMA
        cols = 2 * HEAD
        step_o = min(dim, 512)
        y = pl.pallas_call(
            functools.partial(_kernel, side),
            out_shape=jax.ShapeDtypeStruct((own, dim), wide),
            in_specs=[any_, vmem, vmem, any_, any_, any_, any_],
            out_specs=any_,
            scratch_shapes=[
                pltpu.VMEM((own, dim), low),
                pltpu.VMEM((own, dim), low),
                pltpu.VMEM((own, HEAD), wide),
                pltpu.VMEM((own, HEAD), wide),
                pltpu.VMEM((SLOTS, dim, group), low),
                pltpu.VMEM((2 * dim // step_o, nu, cols, step_o), low),
                pltpu.VMEM((nu, 2 * HEAD, own), low),
                pltpu.VMEM((total, 2 * HEAD, own), low),
                pltpu.VMEM((nu, 2, own, cols), low),
                pltpu.VMEM((nu, 2, own, cols), low),
                pltpu.VMEM((nu, CORES, own, cols), low),
                pltpu.VMEM((2, nu, own, cols), low),
                pltpu.VMEM((own, dim), wide),
                pltpu.VMEM((nu, CORES, cols), wide),
                pltpu.VMEM((nu, CORES, cols), wide),
                pltpu.VMEM((nu, CORES, HEAD + 8, cols), wide),
                pltpu.VMEM((CORES, side * CORES * own, cols), wide),
                dma, dma((SLOTS, 2)), dma((2 * dim // step_o,)),
                dma((nu,)), dma((nu,)), dma((3, 4)), dma((3, 4)),
                dma((nu,)), dma((nu,)), dma((nu, CORES)), dma((2, nu)),
            ],
            compiler_params=pltpu.CompilerParams(collective_id=0, has_side_effects=True, vmem_limit_bytes=63 * 2**20),
        )(x, gain.reshape(-1, HEAD), rate, wq, wk, wv, wo.reshape(nu, 2, cols, dim))
        return (x.astype(wide) + y).astype(low)

    tokens, whole = P(("dp", "sp"), None), P(None, None)
    return jax.shard_map(
        step,
        mesh=mesh,
        in_specs=(tokens, P(None), whole, whole, whole, whole),
        out_specs=tokens,
        check_vma=False,
    )
```

```python
import functools
import math

import jax
import jax.numpy as jnp
from jax import lax
from jax.experimental import pallas as pl
from jax.experimental.pallas import tpu as pltpu
from jax.sharding import PartitionSpec as P

HEAD = 128
THETA = 10000
CORES = 2
NEG = -1e30
HIDDEN = 2 * NEG
LOG2E = 1.4426950408889634
SLOTS = 3
MESH = pl.DeviceIdType.MESH
PASSES = [[], [], [(0, 2)], [(0, 1)], [(0, 3)], [(1, 0)], [], [(1, 2)]]


def _dot(a, b, ca=1, cb=0):
    return lax.dot_general(a, b, (((ca,), (cb,)), ((), ())), preferred_element_type=jnp.float32)


def _kernel(side, x_hbm, gain_ref, rate_ref, wq, wk, wv, wo, y_hbm,
            xv, av, cos_ref, sin_ref, wbuf, wobuf, kvs, kvg, qs, qg, os, og, acc, top_s, keep_s, mix_s, s_s,
            x_sem, w_sem, wo_sem, kv_send, kv_recv, g_send, g_recv, q_send, q_recv, o_send, o_recv):
    own, dim = xv.shape
    nc = 4
    nu = nc * CORES
    cols = 2 * HEAD
    group = 2 * cols
    me = lax.axis_index("sp")
    x, y, c = lax.div(me, CORES * side), lax.rem(lax.div(me, CORES), side), lax.rem(me, CORES)
    hx, hy = lax.div(x, 2), lax.div(y, 2)
    gx, gy = lax.rem(x + hx, 2), lax.rem(y + hy, 2)
    u = (hx * 2 + hy) * CORES + c

    def flip(a, d, top=1):
        return a + d * (top - 2 * a)

    def dev(xx, yy, cc):
        return {"sp": (xx * side + yy) * CORES + cc}

    def remote(src, dst, send, recv, to):
        return pltpu.make_async_remote_copy(src_ref=src, dst_ref=dst, send_sem=send, recv_sem=recv, device_id=to, device_id_type=MESH)

    def other(n):
        dx, dy = lax.rem(n, 2), lax.rem(lax.div(n + 1, 2), 2)
        return flip(x, dx, side - 1), flip(y, dy, side - 1), flip(hx, dx) * 2 + flip(hy, dy)

    def place(i, fx=0, fy=0):
        ax, ay = flip(gx, fx), flip(gy, fy)
        return flip(ax, i // 2, side - 1), flip(ay, i % 2, side - 1)

    def beside(a):
        return a + 1 - 2 * lax.rem(a, 2)

    def load_kv(n):
        _, _, chip = other(jnp.int32(n))
        wide = CORES * HEAD
        at = pl.ds(pl.multiple_of(chip * wide, wide), wide)
        return [pltpu.make_async_copy(wk.at[:, at], wbuf.at[n % SLOTS, :, pl.ds(0, wide)], w_sem.at[n % SLOTS, 0]),
                pltpu.make_async_copy(wv.at[:, at], wbuf.at[n % SLOTS, :, pl.ds(wide, wide)], w_sem.at[n % SLOTS, 1])]

    def target(j):
        xx, yy, chip = other(lax.rem(lax.div(j, CORES) + 1, nc))
        cc = flip(c, 1 - lax.rem(j, CORES))
        return xx, yy, cc, chip * CORES + cc

    def load_q(j):
        at = pl.ds(pl.multiple_of(target(j)[3] * group, group), group)
        slot = lax.rem(j + nc, SLOTS)
        return pltpu.make_async_copy(wq.at[:, at], wbuf.at[slot], w_sem.at[slot, 0])

    step = wobuf.shape[3]
    slabs = dim // step

    def load_o(p, n):
        at = pl.ds(pl.multiple_of(n * step, step), step)
        return pltpu.make_async_copy(wo.at[:, p, :, at], wobuf.at[p * slabs + n], wo_sem.at[p * slabs + n])

    get_x = pltpu.make_async_copy(x_hbm, xv, x_sem)
    get_x.start()
    for copy in load_kv(0):
        copy.start()

    barrier = pltpu.get_barrier_semaphore()
    peers = [dev(flip(x, dx, side - 1), flip(y, dy, side - 1), flip(c, dc)) for dx in range(2) for dy in range(2) for dc in range(2) if dx + dy + dc]
    near = [(beside(x), y), (x, beside(y))]
    peers += [dev(xx, yy, c) for xx, yy in near]
    for peer in peers:
        pl.semaphore_signal(barrier, inc=1, device_id=peer, device_id_type=MESH)

    place_ = (me * own + lax.broadcasted_iota(jnp.int32, (own, HEAD), 0)).astype(jnp.float32)
    angle = place_ * rate_ref[...]
    second = lax.broadcasted_iota(jnp.int32, (own, HEAD), 1) >= HEAD // 2
    cos_ref[...] = jnp.cos(angle)
    sin_ref[...] = jnp.where(second, jnp.sin(angle), -jnp.sin(angle))
    for n in range(1, SLOTS):
        for copy in load_kv(n):
            copy.start()
    with jax.named_scope("wait_x"):
        get_x.wait()
    wide = xv[...].astype(jnp.float32)
    scale = lax.rsqrt(jnp.mean(wide * wide, -1, keepdims=True) + 1e-6)
    lanes = gain_ref.shape[1]
    for k in range(dim // lanes):
        at = slice(k * lanes, (k + 1) * lanes)
        av[:, at] = (xv[:, at].astype(jnp.float32) * scale * gain_ref[k : k + 1, :].astype(jnp.float32)).astype(jnp.bfloat16)
    with jax.named_scope("wait_b"):
        pl.semaphore_wait(barrier, len(peers))

    def turn(t):
        t = t.astype(jnp.float32)
        return (t * cos_ref[...] + pltpu.roll(t, HEAD // 2, 1) * sin_ref[...]).astype(jnp.bfloat16)

    def chip_block(xx, yy):
        return kvg.at[pl.ds((xx * side + yy) * CORES, CORES)]

    def passed(d, i):
        block = chip_block(*place(i))
        return remote(block, block, g_send.at[d, i], g_recv.at[d, i], dev(*near[d], c))

    def relayed(i):
        odd = lax.rem(i, 2)
        block = chip_block(*place(i, odd, 1 - odd))
        (ax, ay), (bx, by) = near
        return remote(block, block, g_send.at[2, i], g_recv.at[2, i], dev(ax + odd * (bx - ax), ay + odd * (by - ay), c))

    def arrived(d, i):
        with jax.named_scope("wait_kvg"):
            block = chip_block(*place(i, int(d != 1), int(d != 0)))
            pltpu.make_async_copy(block, block, g_recv.at[d, i]).wait()

    def relay(i):
        odd = lax.rem(i, 2)
        with jax.named_scope("wait_relay"):
            block = chip_block(*place(i, odd, 1 - odd))
            pltpu.make_async_copy(block, block, g_recv.at[1 - odd, i]).wait()
        relayed(i).start()

    def pass_on(i):
        with jax.named_scope("wait_kvx"):
            for h in range(CORES):
                pltpu.make_async_copy(kvs.at[0], kvg.at[dev(*place(i), h)["sp"]], kv_recv.at[i * CORES + h]).wait()
        for d in range(2):
            passed(d, i).start()

    def turn_to(n):
        _, _, chip = other(jnp.int32(n))
        return chip

    for n in range(nc):
        with jax.named_scope("wait_wkv"):
            for copy in load_kv(n):
                copy.wait()
        both = _dot(av[...], wbuf[n % SLOTS]).astype(jnp.bfloat16)
        if n + SLOTS < nc:
            for copy in load_kv(n + SLOTS):
                copy.start()
        else:
            load_q(jnp.int32(n + SLOTS - nc)).start()
        xx, yy, _ = other(jnp.int32(n))
        for h in range(CORES):
            i = n * CORES + h
            kvs[i, :HEAD, :] = turn(both[:, h * HEAD : (h + 1) * HEAD])
            at = (CORES + h) * HEAD
            kvs[i, HEAD:, :] = both[:, at : at + HEAD].T
            there = remote(kvs.at[i], kvg.at[me], kv_send.at[i], kv_recv.at[u], dev(xx, yy, h))
            if n > 0:
                there.start()
            else:
                here = pltpu.make_async_copy(kvs.at[i], kvg.at[me], kv_recv.at[u])
                pl.when(c == h)(here.start)
                pl.when(c != h)(there.start)
        if n == 1:
            pass_on(turn_to(0))

    def queries(j, _):
        with jax.named_scope("wait_wq"):
            load_q(j).wait()
        slot = lax.rem(j + nc, SLOTS)
        t = _dot(av[...], wbuf[slot]).astype(jnp.bfloat16)

        @pl.when(j + SLOTS < nu)
        def _():
            load_q(j + SLOTS).start()

        @pl.when(j + SLOTS >= nu)
        def _():
            load_o(0, j + SLOTS - nu).start()

        for p in range(2):
            for s in range(2):
                at = p * cols + s * HEAD
                qs[j, p, :, s * HEAD : (s + 1) * HEAD] = turn(t[:, at : at + HEAD])
        xx, yy, cc, _ = target(j)
        here = pltpu.make_async_copy(qs.at[j], qg.at[u], q_recv.at[u])
        there = remote(qs.at[j], qg.at[u], q_send.at[j], q_recv.at[u], dev(xx, yy, cc))
        pl.when(j == nu - 1)(here.start)
        pl.when(j < nu - 1)(there.start)

        for at, do in enumerate(PASSES):
            for f, i in do:
                pl.when(j == at)(functools.partial((pass_on, relay)[f], turn_to(i)))

    lax.fori_loop(0, nu, queries, None)
    for n in range(SLOTS, slabs):
        load_o(0, n).start()
    for n in range(slabs):
        load_o(1, n).start()

    e = HEAD**-0.5 * LOG2E
    row = side * CORES
    bk = row * HEAD

    def of(n):
        return lax.rem(n, 4), lax.div(n, 4)

    def raw_score(i, n, t):
        chip, p = of(n)
        k = jnp.concatenate([kvg[t * row + a, :HEAD, :] for a in range(row)], axis=0)
        q = qg[chip * CORES + i, p]
        q = jnp.concatenate([q[:, :HEAD], q[:, HEAD:]], axis=0)
        return _dot(k, q, 1, 1)

    def settle(i, s, room, old):
        if room is not None:
            gap = lax.rem(lax.broadcasted_iota(jnp.int32, (bk, cols), 1), HEAD) - lax.broadcasted_iota(jnp.int32, (bk, cols), 0)
            s = jnp.where(gap >= -(room + i * HEAD), s, HIDDEN)
        top = jnp.maximum(old, s.max(axis=0, keepdims=True))
        s_s[i] = s
        return top, jnp.exp2((old - top) * e)

    def score(i, n, t, room, old):
        return settle(i, raw_score(i, n, t), room, old)

    def weights(i, top):
        return jnp.exp2((s_s[i] - top) * e).astype(jnp.bfloat16)

    def mixed(i, t, w, keep, n):
        v = jnp.concatenate([kvg[t * row + a, HEAD:, :] for a in range(row)], axis=1)
        v = jnp.concatenate([v, jnp.ones((8, bk), jnp.bfloat16)], axis=0)
        mix_s[n, i] = mix_s[n, i] * keep + _dot(v, w)

    def weigh(i, t, top, keep, n):
        mixed(i, t, weights(i, top), keep, n)

    def note(n, parts):
        for i, (top, keep) in enumerate(parts):
            top_s[n, i : i + 1, :] = top
            keep_s[n, i : i + 1, :] = keep

    def noted(ref, n):
        return [ref[n, i : i + 1, :] for i in range(CORES)]

    def room_of(n):
        return place(of(n)[0])[1] * (CORES * HEAD)

    def both(n, t, m, s, masked):
        tops, keeps, olds = noted(top_s, m), noted(keep_s, m), noted(top_s, n)
        room = room_of(n) if masked else None
        raw = [raw_score(i, n, t) for i in range(CORES)]
        for i in range(CORES):
            weigh(i, s, tops[i], keeps[i], m)
        parts = [settle(i, raw[i], room, olds[i]) for i in range(CORES)]
        note(n, parts)

    def sent(n, h, p, qx, qy):
        return remote(os.at[n, h], og.at[p, u], o_send.at[n, h], o_recv.at[p, u], dev(qx, qy, h))

    def finish(n):
        chip, p = of(n)
        qx, qy = place(chip)
        for i in range(CORES):
            done = (mix_s[n, i, :HEAD, :] * (1 / mix_s[n, i, HEAD : HEAD + 1, :])).astype(jnp.bfloat16)
            for s in range(2):
                os[n, i, :, s * HEAD : (s + 1) * HEAD] = done[:, s * HEAD : (s + 1) * HEAD].T
        for h in range(CORES):
            mine = (chip * CORES + h) == u
            pl.when(mine)(pltpu.make_async_copy(os.at[n, h], og.at[p, u], o_recv.at[p, u]).start)
            pl.when(jnp.logical_not(mine))(sent(n, h, p, qx, qy).start)

    def take_q(chip):
        with jax.named_scope("wait_q"):
            for h in range(CORES):
                pltpu.make_async_copy(qs.at[0], qg.at[chip * CORES + h], q_recv.at[chip * CORES + h]).wait()

    top_s[...] = jnp.full(top_s.shape, NEG, jnp.float32)
    mix_s[...] = jnp.zeros(mix_s.shape, jnp.float32)
    zero = jnp.int32(0)
    relay(turn_to(1))
    relay(turn_to(3))
    arrived(1, 1)
    take_q(zero)
    note(zero, [score(i, zero, gx, room_of(zero), old) for i, old in enumerate(noted(top_s, zero))])

    def attend(g, before):
        m, s = before
        p, r = lax.div(g, 10), lax.rem(g, 10)
        k = r - 2 - 2 * gx
        per = 4 - gx
        far = lax.div(r + 8 - 2 * gx, 10)
        chip_far, t_far = 2 + lax.div(k + per, per) - 1, lax.rem(k + per, per)
        chip_near, t_near = lax.div(r, 1 + gx), gx * (1 - lax.rem(r, 2))
        t_far0 = t_far + lax.div(t_far, 2) * (1 - 2 * lax.rem(t_far, 2))
        t_far1 = t_far + (1 - lax.div(t_far, 2)) * (1 - 2 * t_far)
        t_far = t_far0 + gx * (t_far1 - t_far0)
        chip, t = chip_near + far * (chip_far - chip_near), t_near + far * (t_far - t_near)
        n = p * 4 + chip
        own = gx + far * (side - 1 - 2 * gx)

        @pl.when(g == 3 - 2 * gx)
        def _():
            for d, i in ((0, 0), (2, 0), (2, 1)):
                arrived(d, i)

        @pl.when(g == 4 + 2 * gx)
        def _():
            arrived(1, 3)

        @pl.when((g == 5) & (gx == 0))
        def _():
            last_gather()

        @pl.when((p == 0) & (r - 1 - gx == 0))
        def _():
            take_q(zero + 1)

        @pl.when((p == 0) & (k == 0))
        def _():
            take_q(zero + 2)

        @pl.when((p == 0) & (k == per))
        def _():
            take_q(zero + 3)

        with jax.named_scope("at"):
            pl.when(t == own)(lambda: both(n, t, m, s, True))
            pl.when(t != own)(lambda: both(n, t, m, s, False))
        pl.when(s == 2 * lax.div(lax.rem(m, 4), 2))(lambda: finish(m))
        return n, t

    def last_gather():
        for d, i in ((0, 2), (2, 2), (2, 3)):
            arrived(d, i)

    at = lax.fori_loop(1, 20, attend, (zero, gx))
    for i in range(CORES):
        weigh(i, at[1], noted(top_s, at[0])[i], noted(keep_s, at[0])[i], at[0])
    finish(at[0])

    for p in range(2):
        with jax.named_scope("wait_o"):
            for k in range(nu):
                pltpu.make_async_copy(os.at[0, 0], og.at[p, k], o_recv.at[p, k]).wait()

        with jax.named_scope("wait_wo"):
            for n in range(slabs):
                load_o(p, n).wait()
        with jax.named_scope("wo"):
            for n in range(slabs):
                more = _dot(og[p, 0], wobuf[p * slabs + n, 0])
                for k in range(1, nu):
                    more += _dot(og[p, k], wobuf[p * slabs + n, k])
                if p == 0:
                    acc[:, n * step : (n + 1) * step] = more
                else:
                    acc[:, n * step : (n + 1) * step] += more
    put = pltpu.make_async_copy(acc, y_hbm, x_sem)
    put.start()

    for n in range(nc):
        xx, yy, _ = other(jnp.int32(n))
        for h in range(CORES):
            i = n * CORES + h
            wait = remote(kvs.at[i], kvg.at[me], kv_send.at[i], kv_recv.at[u], dev(xx, yy, h)).wait_send
            if n > 0:
                wait()
            else:
                pl.when(c != h)(wait)
    for i in range(nc):
        for d in range(2):
            passed(d, i).wait_send()
        relayed(i).wait_send()

    def left(n, _):
        xx, yy, cc, _ = target(n)
        pl.when(n < nu - 1)(remote(qs.at[n], qg.at[u], q_send.at[n], q_recv.at[u], dev(xx, yy, cc)).wait_send)
        chip, p = of(n)
        for h in range(CORES):
            pl.when(chip * CORES + h != u)(sent(n, h, p, *place(chip)).wait_send)

    lax.fori_loop(0, nu, left, None)
    pl.when(gx == 1)(last_gather)
    put.wait()


def solution(mesh):
    total = mesh.shape["sp"]

    def step(x, gain, wq, wk, wv, wo):
        own, dim = x.shape
        nu = wk.shape[1] // HEAD
        side = math.isqrt(total // CORES)
        group = wq.shape[1] // nu
        half = HEAD // 2
        rate = THETA ** (-jnp.arange(half, dtype=jnp.float32) / half)
        rate = jnp.concatenate([rate, rate])[None]
        any_ = pl.BlockSpec(memory_space=pltpu.HBM)
        vmem = pl.BlockSpec(memory_space=pltpu.VMEM)
        low, wide = jnp.bfloat16, jnp.float32
        dma = pltpu.SemaphoreType.DMA
        cols = 2 * HEAD
        step_o = min(dim, 512)
        y = pl.pallas_call(
            functools.partial(_kernel, side),
            out_shape=jax.ShapeDtypeStruct((own, dim), wide),
            in_specs=[any_, vmem, vmem, any_, any_, any_, any_],
            out_specs=any_,
            scratch_shapes=[
                pltpu.VMEM((own, dim), low),
                pltpu.VMEM((own, dim), low),
                pltpu.VMEM((own, HEAD), wide),
                pltpu.VMEM((own, HEAD), wide),
                pltpu.VMEM((SLOTS, dim, group), low),
                pltpu.VMEM((2 * dim // step_o, nu, cols, step_o), low),
                pltpu.VMEM((nu, 2 * HEAD, own), low),
                pltpu.VMEM((total, 2 * HEAD, own), low),
                pltpu.VMEM((nu, 2, own, cols), low),
                pltpu.VMEM((nu, 2, own, cols), low),
                pltpu.VMEM((nu, CORES, own, cols), low),
                pltpu.VMEM((2, nu, own, cols), low),
                pltpu.VMEM((own, dim), wide),
                pltpu.VMEM((nu, CORES, cols), wide),
                pltpu.VMEM((nu, CORES, cols), wide),
                pltpu.VMEM((nu, CORES, HEAD + 8, cols), wide),
                pltpu.VMEM((CORES, side * CORES * own, cols), wide),
                dma, dma((SLOTS, 2)), dma((2 * dim // step_o,)),
                dma((nu,)), dma((nu,)), dma((3, 4)), dma((3, 4)),
                dma((nu,)), dma((nu,)), dma((nu, CORES)), dma((2, nu)),
            ],
            compiler_params=pltpu.CompilerParams(collective_id=0, has_side_effects=True, vmem_limit_bytes=63 * 2**20),
        )(x, gain.reshape(-1, HEAD), rate, wq, wk, wv, wo.reshape(nu, 2, cols, dim))
        return (x.astype(wide) + y).astype(low)

    tokens, whole = P(("dp", "sp"), None), P(None, None)
    return jax.shard_map(
        step,
        mesh=mesh,
        in_specs=(tokens, P(None), whole, whole, whole, whole),
        out_specs=tokens,
        check_vma=False,
    )
```

```python
import functools
import math

import jax
import jax.numpy as jnp
from jax import lax
from jax.experimental import pallas as pl
from jax.experimental.pallas import tpu as pltpu
from jax.sharding import PartitionSpec as P

HEAD = 128
THETA = 10000
CORES = 2
NEG = -1e30
HIDDEN = 2 * NEG
LOG2E = 1.4426950408889634
SLOTS = 3
MESH = pl.DeviceIdType.MESH
VMEM = 63 * 2**20
PASSES = [[], [], [(0, 2)], [(0, 1)], [(0, 3)], [(1, 0)], [], [(1, 2)]]


def _dot(a, b, ca=1, cb=0):
    return lax.dot_general(a, b, (((ca,), (cb,)), ((), ())), preferred_element_type=jnp.float32)


def _kernel(side, x_hbm, gain_ref, rate_ref, wq, wk, wv, wo, y_ref,
            xv, av, cos_ref, sin_ref, wbuf, wobuf, kvs, kvg, qs, qg, os, og, acc, top_s, keep_s, mix_s, s_s,
            x_sem, w_sem, wo_sem, kv_send, kv_recv, g_send, g_recv, q_send, q_recv, o_send, o_recv):
    own, dim = xv.shape
    nc = 4
    nu = nc * CORES
    cols = 2 * HEAD
    group = 2 * cols
    me = lax.axis_index("sp")
    x, y, c = lax.div(me, CORES * side), lax.rem(lax.div(me, CORES), side), lax.rem(me, CORES)
    hx, hy = lax.div(x, 2), lax.div(y, 2)
    gx, gy = lax.rem(x + hx, 2), lax.rem(y + hy, 2)
    u = (hx * 2 + hy) * CORES + c

    def flip(a, d, top=1):
        return a + d * (top - 2 * a)

    def dev(xx, yy, cc):
        return {"sp": (xx * side + yy) * CORES + cc}

    def remote(src, dst, send, recv, to):
        return pltpu.make_async_remote_copy(src_ref=src, dst_ref=dst, send_sem=send, recv_sem=recv, device_id=to, device_id_type=MESH)

    def other(n):
        dx, dy = lax.rem(n, 2), lax.rem(lax.div(n + 1, 2), 2)
        return flip(x, dx, side - 1), flip(y, dy, side - 1), flip(hx, dx) * 2 + flip(hy, dy)

    def place(i, fx=0, fy=0):
        ax, ay = flip(gx, fx), flip(gy, fy)
        return flip(ax, i // 2, side - 1), flip(ay, i % 2, side - 1)

    def beside(a):
        return a + 1 - 2 * lax.rem(a, 2)

    def load_kv(n):
        _, _, chip = other(jnp.int32(n))
        wide = CORES * HEAD
        at = pl.ds(pl.multiple_of(chip * wide, wide), wide)
        return [pltpu.make_async_copy(wk.at[:, at], wbuf.at[n % SLOTS, :, pl.ds(0, wide)], w_sem.at[n % SLOTS, 0]),
                pltpu.make_async_copy(wv.at[:, at], wbuf.at[n % SLOTS, :, pl.ds(wide, wide)], w_sem.at[n % SLOTS, 1])]

    def target(j):
        xx, yy, chip = other(lax.rem(lax.div(j, CORES) + 1, nc))
        cc = flip(c, 1 - lax.rem(j, CORES))
        return xx, yy, cc, chip * CORES + cc

    def load_q(j):
        at = pl.ds(pl.multiple_of(target(j)[3] * group, group), group)
        slot = lax.rem(j + nc, SLOTS)
        return pltpu.make_async_copy(wq.at[:, at], wbuf.at[slot], w_sem.at[slot, 0])

    step = wobuf.shape[3]
    slabs = dim // step

    def load_o(p, n):
        at = pl.ds(pl.multiple_of(n * step, step), step)
        return pltpu.make_async_copy(wo.at[:, p, :, at], wobuf.at[p * slabs + n], wo_sem.at[p * slabs + n])

    get_x = pltpu.make_async_copy(x_hbm, xv, x_sem)
    get_x.start()
    for copy in load_kv(0):
        copy.start()

    barrier = pltpu.get_barrier_semaphore()
    peers = [dev(flip(x, dx, side - 1), flip(y, dy, side - 1), flip(c, dc)) for dx in range(2) for dy in range(2) for dc in range(2) if dx + dy + dc]
    near = [(beside(x), y), (x, beside(y))]
    peers += [dev(xx, yy, c) for xx, yy in near]
    for peer in peers:
        pl.semaphore_signal(barrier, inc=1, device_id=peer, device_id_type=MESH)

    place_ = (me * own + lax.broadcasted_iota(jnp.int32, (own, HEAD), 0)).astype(jnp.float32)
    angle = place_ * rate_ref[...]
    second = lax.broadcasted_iota(jnp.int32, (own, HEAD), 1) >= HEAD // 2
    cos_ref[...] = jnp.cos(angle)
    sin_ref[...] = jnp.where(second, jnp.sin(angle), -jnp.sin(angle))
    for n in range(1, SLOTS):
        for copy in load_kv(n):
            copy.start()
    with jax.named_scope("wait_x"):
        get_x.wait()
    wide = xv[...].astype(jnp.float32)
    scale = lax.rsqrt(jnp.mean(wide * wide, -1, keepdims=True) + 1e-6)
    lanes = gain_ref.shape[1]
    for k in range(dim // lanes):
        at = slice(k * lanes, (k + 1) * lanes)
        av[:, at] = (xv[:, at].astype(jnp.float32) * scale * gain_ref[k : k + 1, :].astype(jnp.float32)).astype(jnp.bfloat16)
    with jax.named_scope("wait_b"):
        pl.semaphore_wait(barrier, len(peers))

    def turn(t):
        t = t.astype(jnp.float32)
        return (t * cos_ref[...] + pltpu.roll(t, HEAD // 2, 1) * sin_ref[...]).astype(jnp.bfloat16)

    def chip_block(xx, yy):
        return kvg.at[pl.ds((xx * side + yy) * CORES, CORES)]

    def passed(d, i):
        block = chip_block(*place(i))
        return remote(block, block, g_send.at[d, i], g_recv.at[d, i], dev(*near[d], c))

    def relayed(i):
        odd = lax.rem(i, 2)
        block = chip_block(*place(i, odd, 1 - odd))
        (ax, ay), (bx, by) = near
        return remote(block, block, g_send.at[2, i], g_recv.at[2, i], dev(ax + odd * (bx - ax), ay + odd * (by - ay), c))

    def arrived(d, i):
        with jax.named_scope("wait_kvg"):
            block = chip_block(*place(i, int(d != 1), int(d != 0)))
            pltpu.make_async_copy(block, block, g_recv.at[d, i]).wait()

    def relay(i):
        odd = lax.rem(i, 2)
        with jax.named_scope("wait_relay"):
            block = chip_block(*place(i, odd, 1 - odd))
            pltpu.make_async_copy(block, block, g_recv.at[1 - odd, i]).wait()
        relayed(i).start()

    def pass_on(i):
        with jax.named_scope("wait_kvx"):
            for h in range(CORES):
                pltpu.make_async_copy(kvs.at[0], kvg.at[dev(*place(i), h)["sp"]], kv_recv.at[i * CORES + h]).wait()
        for d in range(2):
            passed(d, i).start()

    def turn_to(n):
        _, _, chip = other(jnp.int32(n))
        return chip

    for n in range(nc):
        with jax.named_scope("wait_wkv"):
            for copy in load_kv(n):
                copy.wait()
        both = _dot(av[...], wbuf[n % SLOTS]).astype(jnp.bfloat16)
        if n + SLOTS < nc:
            for copy in load_kv(n + SLOTS):
                copy.start()
        else:
            load_q(jnp.int32(n + SLOTS - nc)).start()
        xx, yy, _ = other(jnp.int32(n))
        for h in range(CORES):
            i = n * CORES + h
            kvs[i, :HEAD, :] = turn(both[:, h * HEAD : (h + 1) * HEAD])
            at = (CORES + h) * HEAD
            kvs[i, HEAD:, :] = both[:, at : at + HEAD].T
            there = remote(kvs.at[i], kvg.at[me], kv_send.at[i], kv_recv.at[u], dev(xx, yy, h))
            if n > 0:
                there.start()
            else:
                here = pltpu.make_async_copy(kvs.at[i], kvg.at[me], kv_recv.at[u])
                pl.when(c == h)(here.start)
                pl.when(c != h)(there.start)
        if n == 1:
            pass_on(turn_to(0))

    def queries(j, _):
        with jax.named_scope("wait_wq"):
            load_q(j).wait()
        slot = lax.rem(j + nc, SLOTS)
        t = _dot(av[...], wbuf[slot]).astype(jnp.bfloat16)

        @pl.when(j + SLOTS < nu)
        def _():
            load_q(j + SLOTS).start()

        @pl.when(j + SLOTS >= nu)
        def _():
            load_o(0, j + SLOTS - nu).start()

        for p in range(2):
            for s in range(2):
                at = p * cols + s * HEAD
                qs[j, p, :, s * HEAD : (s + 1) * HEAD] = turn(t[:, at : at + HEAD])
        xx, yy, cc, _ = target(j)
        here = pltpu.make_async_copy(qs.at[j], qg.at[u], q_recv.at[u])
        there = remote(qs.at[j], qg.at[u], q_send.at[j], q_recv.at[u], dev(xx, yy, cc))
        pl.when(j == nu - 1)(here.start)
        pl.when(j < nu - 1)(there.start)

        for at, do in enumerate(PASSES):
            for f, i in do:
                pl.when(j == at)(functools.partial((pass_on, relay)[f], turn_to(i)))

    lax.fori_loop(0, nu, queries, None)
    for n in range(SLOTS, slabs):
        load_o(0, n).start()
    for n in range(slabs):
        load_o(1, n).start()

    e = HEAD**-0.5 * LOG2E
    row = side * CORES
    bk = row * HEAD

    def of(n):
        return lax.rem(lax.div(n, 2), 2), lax.rem(n, 2), lax.div(n, 4)

    def raw_score(i, n, t):
        far, h, p = of(n)
        k = jnp.concatenate([kvg[t * row + a, :HEAD, :] for a in range(row)], axis=0)
        q = qg[(far * 2 + i) * CORES + h, p]
        q = jnp.concatenate([q[:, :HEAD], q[:, HEAD:]], axis=0)
        return _dot(k, q, 1, 1)

    def settle(i, s, room, old):
        if room is not None:
            gap = lax.rem(lax.broadcasted_iota(jnp.int32, (bk, cols), 1), HEAD) - lax.broadcasted_iota(jnp.int32, (bk, cols), 0)
            s = jnp.where(gap >= -room[i], s, HIDDEN)
        top = jnp.maximum(old, s.max(axis=0, keepdims=True))
        s_s[i] = s
        return top, jnp.exp2((old - top) * e)

    def score(i, n, t, room, old):
        return settle(i, raw_score(i, n, t), room, old)

    def weights(i, top):
        return jnp.exp2((s_s[i] - top) * e).astype(jnp.bfloat16)

    def mixed(i, t, w, keep):
        v = jnp.concatenate([kvg[t * row + a, HEAD:, :] for a in range(row)], axis=1)
        v = jnp.concatenate([v, jnp.ones((8, bk), jnp.bfloat16)], axis=0)
        mix_s[i] = mix_s[i] * keep + _dot(v, w)

    def weigh(i, t, top, keep):
        mixed(i, t, weights(i, top), keep)

    def note(n, parts):
        for i, (top, keep) in enumerate(parts):
            top_s[n, i : i + 1, :] = top
            keep_s[n, i : i + 1, :] = keep

    def noted(ref, n):
        return [ref[n, i : i + 1, :] for i in range(CORES)]

    def room_of(n):
        far, h, _ = of(n)
        return [(place(far * 2 + i)[1] * CORES + h) * HEAD for i in range(2)]

    def both(n, t, m, s, masked):
        tops, keeps, olds = noted(top_s, m), noted(keep_s, m), noted(top_s, n)
        room = room_of(n) if masked else None
        raw = [raw_score(i, n, t) for i in range(CORES)]
        for i in range(CORES):
            weigh(i, s, tops[i], keeps[i])
        parts = [settle(i, raw[i], room, olds[i]) for i in range(CORES)]
        note(n, parts)

    def sent(n, i):
        far, h, p = of(n)
        return remote(os.at[n, i], og.at[p, u], o_send.at[n, i], o_recv.at[p, u], dev(*place(far * 2 + i), h))

    def finish(n):
        far, h, p = of(n)
        for i in range(2):
            done = (mix_s[i, :HEAD, :] * (1 / mix_s[i, HEAD : HEAD + 1, :])).astype(jnp.bfloat16)
            for s in range(2):
                os[n, i, :, s * HEAD : (s + 1) * HEAD] = done[:, s * HEAD : (s + 1) * HEAD].T
        for i in range(2):
            mine = (far * 2 + i) * CORES + h == u
            pl.when(mine)(pltpu.make_async_copy(os.at[n, i], og.at[p, u], o_recv.at[p, u]).start)
            pl.when(jnp.logical_not(mine))(sent(n, i).start)

    def take_q(n):
        far, h, _ = of(n)
        with jax.named_scope("wait_q"):
            for i in range(2):
                at = (far * 2 + i) * CORES + h
                pltpu.make_async_copy(qs.at[0], qg.at[at], q_recv.at[at]).wait()

    top_s[...] = jnp.full(top_s.shape, NEG, jnp.float32)
    mix_s[...] = jnp.zeros(mix_s.shape, jnp.float32)
    zero = jnp.int32(0)

    @pl.when(hx == 1)
    def _():
        relay(turn_to(1))
        relay(turn_to(3))

    arrived(1, 1)
    take_q(zero)
    note(zero, [score(i, zero, gx, room_of(zero), old) for i, old in enumerate(noted(top_s, zero))])

    def attend(g, before):
        m, s = before
        p, r = lax.div(g, 10), lax.rem(g, 10)
        k = r - 2 - 2 * gx
        per = 4 - gx
        far = lax.div(r + 8 - 2 * gx, 10)
        item_far, t_far = 2 + lax.div(k + per, per) - 1, lax.rem(k + per, per)
        item_near, t_near = lax.div(r, 1 + gx), gx * (1 - lax.rem(r, 2))
        t_far0 = t_far + lax.div(t_far, 2) * (1 - 2 * lax.rem(t_far, 2))
        t_far1 = t_far + (1 - lax.div(t_far, 2)) * (1 - 2 * t_far)
        t_far = t_far0 + gx * (t_far1 - t_far0)
        item, t = item_near + far * (item_far - item_near), t_near + far * (t_far - t_near)
        n = p * 4 + item
        own = gx + far * (side - 1 - 2 * gx)

        pl.when((g == 1) & (hx == 0))(lambda: relay(turn_to(1)))
        pl.when((g == 2) & (hx == 0))(lambda: relay(turn_to(3)))

        @pl.when(g == 3 - 2 * gx)
        def _():
            for d, i in ((0, 0), (2, 0), (2, 1)):
                arrived(d, i)

        @pl.when(g == 4 + 2 * gx)
        def _():
            arrived(1, 3)

        @pl.when((g == 5) & (gx == 0))
        def _():
            last_gather()

        @pl.when((p == 0) & (r - 1 - gx == 0))
        def _():
            take_q(zero + 1)

        @pl.when((p == 0) & (k == 0))
        def _():
            take_q(zero + 2)

        @pl.when((p == 0) & (k == per))
        def _():
            take_q(zero + 3)

        with jax.named_scope("at"):
            pl.when(t == own)(lambda: both(n, t, m, s, True))
            pl.when(t != own)(lambda: both(n, t, m, s, False))
        pl.when(s == 2 * lax.div(lax.rem(m, 4), 2))(lambda: finish(m))
        return n, t

    def last_gather():
        for d, i in ((0, 2), (2, 2), (2, 3)):
            arrived(d, i)

    at = lax.fori_loop(1, 20, attend, (zero, gx))
    for i in range(CORES):
        weigh(i, at[1], noted(top_s, at[0])[i], noted(keep_s, at[0])[i])
    finish(at[0])

    for p in range(2):
        with jax.named_scope("wait_o"):
            for k in range(nu):
                pltpu.make_async_copy(os.at[0, 0], og.at[p, k], o_recv.at[p, k]).wait()

        with jax.named_scope("wait_wo"):
            for n in range(slabs):
                load_o(p, n).wait()
        with jax.named_scope("wo"):
            for n in range(slabs):
                more = _dot(og[p, 0], wobuf[p * slabs + n, 0])
                for k in range(1, nu):
                    more += _dot(og[p, k], wobuf[p * slabs + n, k])
                if p == 0:
                    acc[:, n * step : (n + 1) * step] = more + xv[:, n * step : (n + 1) * step].astype(jnp.float32)
                else:
                    y_ref[:, n * step : (n + 1) * step] = (acc[:, n * step : (n + 1) * step] + more).astype(jnp.bfloat16)

    for n in range(nc):
        xx, yy, _ = other(jnp.int32(n))
        for h in range(CORES):
            i = n * CORES + h
            wait = remote(kvs.at[i], kvg.at[me], kv_send.at[i], kv_recv.at[u], dev(xx, yy, h)).wait_send
            if n > 0:
                wait()
            else:
                pl.when(c != h)(wait)
    for i in range(nc):
        for d in range(2):
            passed(d, i).wait_send()
        relayed(i).wait_send()

    def left(n, _):
        xx, yy, cc, _ = target(n)
        pl.when(n < nu - 1)(remote(qs.at[n], qg.at[u], q_send.at[n], q_recv.at[u], dev(xx, yy, cc)).wait_send)
        far, h, _ = of(n)
        for i in range(2):
            pl.when((far * 2 + i) * CORES + h != u)(sent(n, i).wait_send)

    lax.fori_loop(0, nu, left, None)
    pl.when(gx == 1)(last_gather)


def solution(mesh):
    total = mesh.shape["sp"]

    def step(x, gain, wq, wk, wv, wo):
        own, dim = x.shape
        nu = wk.shape[1] // HEAD
        side = math.isqrt(total // CORES)
        group = wq.shape[1] // nu
        half = HEAD // 2
        rate = THETA ** (-jnp.arange(half, dtype=jnp.float32) / half)
        rate = jnp.concatenate([rate, rate])[None]
        any_ = pl.BlockSpec(memory_space=pltpu.HBM)
        vmem = pl.BlockSpec(memory_space=pltpu.VMEM)
        low, wide = jnp.bfloat16, jnp.float32
        dma = pltpu.SemaphoreType.DMA
        cols = 2 * HEAD
        step_o = min(dim, 512)
        y = pl.pallas_call(
            functools.partial(_kernel, side),
            out_shape=jax.ShapeDtypeStruct((own, dim), low),
            in_specs=[any_, vmem, vmem, any_, any_, any_, any_],
            out_specs=vmem,
            scratch_shapes=[
                pltpu.VMEM((own, dim), low),
                pltpu.VMEM((own, dim), low),
                pltpu.VMEM((own, HEAD), wide),
                pltpu.VMEM((own, HEAD), wide),
                pltpu.VMEM((SLOTS, dim, group), low),
                pltpu.VMEM((2 * dim // step_o, nu, cols, step_o), low),
                pltpu.VMEM((nu, 2 * HEAD, own), low),
                pltpu.VMEM((total, 2 * HEAD, own), low),
                pltpu.VMEM((nu, 2, own, cols), low),
                pltpu.VMEM((nu, 2, own, cols), low),
                pltpu.VMEM((nu, CORES, own, cols), low),
                pltpu.VMEM((2, nu, own, cols), low),
                pltpu.VMEM((own, dim), wide),
                pltpu.VMEM((nu, CORES, cols), wide),
                pltpu.VMEM((nu, CORES, cols), wide),
                pltpu.VMEM((CORES, HEAD + 8, cols), wide),
                pltpu.VMEM((CORES, side * CORES * own, cols), wide),
                dma, dma((SLOTS, 2)), dma((2 * dim // step_o,)),
                dma((nu,)), dma((nu,)), dma((3, 4)), dma((3, 4)),
                dma((nu,)), dma((nu,)), dma((nu, CORES)), dma((2, nu)),
            ],
            compiler_params=pltpu.CompilerParams(collective_id=0, has_side_effects=True, vmem_limit_bytes=VMEM),
        )(x, gain.reshape(-1, HEAD), rate, wq, wk, wv, wo.reshape(nu, 2, cols, dim))
        return y

    tokens, whole = P(("dp", "sp"), None), P(None, None)
    return jax.shard_map(
        step,
        mesh=mesh,
        in_specs=(tokens, P(None), whole, whole, whole, whole),
        out_specs=tokens,
        check_vma=False,
    )
```

```python
import functools
import math

import jax
import jax.numpy as jnp
from jax import lax
from jax.experimental import pallas as pl
from jax.experimental.pallas import tpu as pltpu
from jax.sharding import PartitionSpec as P

HEAD = 128
THETA = 10000
CORES = 2
NEG = -1e30
HIDDEN = 2 * NEG
LOG2E = 1.4426950408889634
SLOTS = 3
MESH = pl.DeviceIdType.MESH
VMEM = 63 * 2**20
UNITS = [1, 3, 0, 2]
HOOKS = [
    {1: [("pass", 2)], 4: [("relay", 0)], 6: [("relay", 2)], 7: [("pass", 3)], 8: [("pass", 1)]},
    {1: [("pass", 3)], 2: [("pass", 1)], 6: [("relay", 3)], 8: [("relay", 1), ("pass", 2)]},
]
LATER = [{3: [("relay", 3)], 5: [("relay", 1)]}, {2: [("relay", 0)], 5: [("relay", 2)]}]


def _dot(a, b, ca=1, cb=0):
    return lax.dot_general(a, b, (((ca,), (cb,)), ((), ())), preferred_element_type=jnp.float32)


def _kernel(side, x_hbm, gain_ref, rate_ref, wq, wk, wv, wo, y_ref,
            xv, av, cos_ref, sin_ref, wbuf, wobuf, kvs, kvg, qs, qg, os, og, acc, top_s, keep_s, mix_s, s_s,
            x_sem, w_sem, wo_sem, kv_send, kv_recv, g_send, g_recv, q_send, q_recv, o_send, o_recv):
    own, dim = xv.shape
    nc = 4
    nu = nc * CORES
    cols = 2 * HEAD
    group = 2 * cols
    me = lax.axis_index("sp")
    x, y, c = lax.div(me, CORES * side), lax.rem(lax.div(me, CORES), side), lax.rem(me, CORES)
    hx, hy = lax.div(x, 2), lax.div(y, 2)
    gx, gy = lax.rem(x + hx, 2), lax.rem(y + hy, 2)
    u = (hx * 2 + hy) * CORES + c

    def flip(a, d, top=1):
        return a + d * (top - 2 * a)

    def dev(xx, yy, cc):
        return {"sp": (xx * side + yy) * CORES + cc}

    def remote(src, dst, send, recv, to):
        return pltpu.make_async_remote_copy(src_ref=src, dst_ref=dst, send_sem=send, recv_sem=recv, device_id=to, device_id_type=MESH)

    def other(n):
        dx, dy = lax.rem(n, 2), lax.rem(lax.div(n + 1, 2), 2)
        return flip(x, dx, side - 1), flip(y, dy, side - 1), flip(hx, dx) * 2 + flip(hy, dy)

    def place(i, fx=0, fy=0):
        ax, ay = flip(gx, fx), flip(gy, fy)
        return flip(ax, i // 2, side - 1), flip(ay, i % 2, side - 1)

    def beside(a):
        return a + 1 - 2 * lax.rem(a, 2)

    def load_kv(n):
        _, _, chip = other(jnp.int32(UNITS[n]))
        wide = CORES * HEAD
        at = pl.ds(pl.multiple_of(chip * wide, wide), wide)
        return [pltpu.make_async_copy(wk.at[:, at], wbuf.at[n % SLOTS, :, pl.ds(0, wide)], w_sem.at[n % SLOTS, 0]),
                pltpu.make_async_copy(wv.at[:, at], wbuf.at[n % SLOTS, :, pl.ds(wide, wide)], w_sem.at[n % SLOTS, 1])]

    def target(j):
        xx, yy, chip = other(lax.rem(lax.div(j, CORES) + 1, nc))
        cc = flip(c, 1 - lax.rem(j, CORES))
        return xx, yy, cc, chip * CORES + cc

    def load_q(j):
        at = pl.ds(pl.multiple_of(target(j)[3] * group, group), group)
        slot = lax.rem(j + nc, SLOTS)
        return pltpu.make_async_copy(wq.at[:, at], wbuf.at[slot], w_sem.at[slot, 0])

    step = wobuf.shape[3]
    slabs = dim // step

    def load_o(p, n):
        at = pl.ds(pl.multiple_of(n * step, step), step)
        return pltpu.make_async_copy(wo.at[:, p, :, at], wobuf.at[p * slabs + n], wo_sem.at[p * slabs + n])

    get_x = pltpu.make_async_copy(x_hbm, xv, x_sem)
    get_x.start()
    for copy in load_kv(0):
        copy.start()

    barrier = pltpu.get_barrier_semaphore()
    peers = [dev(flip(x, dx, side - 1), flip(y, dy, side - 1), flip(c, dc)) for dx in range(2) for dy in range(2) for dc in range(2) if dx + dy + dc]
    near = [(beside(x), y), (x, beside(y))]
    peers += [dev(xx, yy, c) for xx, yy in near]
    for peer in peers:
        pl.semaphore_signal(barrier, inc=1, device_id=peer, device_id_type=MESH)

    place_ = (me * own + lax.broadcasted_iota(jnp.int32, (own, HEAD), 0)).astype(jnp.float32)
    angle = place_ * rate_ref[...]
    second = lax.broadcasted_iota(jnp.int32, (own, HEAD), 1) >= HEAD // 2
    cos_ref[...] = jnp.cos(angle)
    sin_ref[...] = jnp.where(second, jnp.sin(angle), -jnp.sin(angle))
    for n in range(1, SLOTS):
        for copy in load_kv(n):
            copy.start()
    with jax.named_scope("wait_x"):
        get_x.wait()
    wide = xv[...].astype(jnp.float32)
    scale = lax.rsqrt(jnp.mean(wide * wide, -1, keepdims=True) + 1e-6)
    lanes = gain_ref.shape[1]
    for k in range(dim // lanes):
        at = slice(k * lanes, (k + 1) * lanes)
        av[:, at] = (xv[:, at].astype(jnp.float32) * scale * gain_ref[k : k + 1, :].astype(jnp.float32)).astype(jnp.bfloat16)
    with jax.named_scope("wait_b"):
        pl.semaphore_wait(barrier, len(peers))

    def turn(t):
        t = t.astype(jnp.float32)
        return (t * cos_ref[...] + pltpu.roll(t, HEAD // 2, 1) * sin_ref[...]).astype(jnp.bfloat16)

    def chip_block(xx, yy):
        return kvg.at[pl.ds((xx * side + yy) * CORES, CORES)]

    def passed(d, i):
        block = chip_block(*place(i))
        return remote(block, block, g_send.at[d, i], g_recv.at[d, i], dev(*near[d], c))

    def relayed(i):
        odd = lax.rem(i, 2)
        block = chip_block(*place(i, odd, 1 - odd))
        (ax, ay), (bx, by) = near
        return remote(block, block, g_send.at[2, i], g_recv.at[2, i], dev(ax + odd * (bx - ax), ay + odd * (by - ay), c))

    def arrived(d, i):
        with jax.named_scope("wait_kvg"):
            block = chip_block(*place(i, int(d != 1), int(d != 0)))
            pltpu.make_async_copy(block, block, g_recv.at[d, i]).wait()

    def relay(i):
        odd = lax.rem(i, 2)
        with jax.named_scope("wait_relay"):
            block = chip_block(*place(i, odd, 1 - odd))
            pltpu.make_async_copy(block, block, g_recv.at[1 - odd, i]).wait()
        relayed(i).start()

    def pass_on(i):
        with jax.named_scope("wait_kvx"):
            for h in range(CORES):
                pltpu.make_async_copy(kvs.at[0], kvg.at[dev(*place(i), h)["sp"]], kv_recv.at[i * CORES + h]).wait()
        for d in range(2):
            passed(d, i).start()

    def turn_to(n):
        _, _, chip = other(jnp.int32(n))
        return chip

    for n in range(nc):
        with jax.named_scope("wait_wkv"):
            for copy in load_kv(n):
                copy.wait()
        both = _dot(av[...], wbuf[n % SLOTS]).astype(jnp.bfloat16)
        if n + SLOTS < nc:
            for copy in load_kv(n + SLOTS):
                copy.start()
        else:
            load_q(jnp.int32(n + SLOTS - nc)).start()
        xx, yy, _ = other(jnp.int32(UNITS[n]))
        for h in range(CORES):
            i = n * CORES + h
            kvs[i, :HEAD, :] = turn(both[:, h * HEAD : (h + 1) * HEAD])
            at = (CORES + h) * HEAD
            kvs[i, HEAD:, :] = both[:, at : at + HEAD].T
            there = remote(kvs.at[i], kvg.at[me], kv_send.at[i], kv_recv.at[u], dev(xx, yy, h))
            if UNITS[n] > 0:
                there.start()
            else:
                here = pltpu.make_async_copy(kvs.at[i], kvg.at[me], kv_recv.at[u])
                pl.when(c == h)(here.start)
                pl.when(c != h)(there.start)
        if n == 3:
            pass_on(turn_to(0))

    def hooks(j, table):
        for half in range(2):
            for at, do in table[half].items():
                if isinstance(j, int) and j != at:
                    continue
                for kind, i in do:
                    act = functools.partial(pass_on if kind == "pass" else relay, turn_to(i))
                    pl.when((j == at) & (hx == half))(act)

    def queries(j, _):
        with jax.named_scope("wait_wq"):
            load_q(j).wait()
        slot = lax.rem(j + nc, SLOTS)
        t = _dot(av[...], wbuf[slot]).astype(jnp.bfloat16)

        @pl.when(j + SLOTS < nu)
        def _():
            load_q(j + SLOTS).start()

        @pl.when(j + SLOTS >= nu)
        def _():
            load_o(0, j + SLOTS - nu).start()

        for p in range(2):
            for s in range(2):
                at = p * cols + s * HEAD
                qs[j, p, :, s * HEAD : (s + 1) * HEAD] = turn(t[:, at : at + HEAD])
        xx, yy, cc, _ = target(j)
        here = pltpu.make_async_copy(qs.at[j], qg.at[u], q_recv.at[u])
        there = remote(qs.at[j], qg.at[u], q_send.at[j], q_recv.at[u], dev(xx, yy, cc))
        pl.when(j == nu - 1)(here.start)
        pl.when(j < nu - 1)(there.start)

        hooks(j, HOOKS)

    lax.fori_loop(0, nu, queries, None)
    hooks(nu, HOOKS)
    for n in range(SLOTS, slabs):
        load_o(0, n).start()
    for n in range(slabs):
        load_o(1, n).start()

    e = HEAD**-0.5 * LOG2E
    row = side * CORES
    bk = row * HEAD

    def of(n):
        return lax.rem(lax.div(n, 2), 2), lax.rem(n, 2), lax.div(n, 4)

    def held(n):
        far, h, p = of(n)
        return (1 - far) * (h + 2 * p) + 4 * far

    def raw_score(i, n, t):
        far, h, p = of(n)
        k = jnp.concatenate([kvg[t * row + a, :HEAD, :] for a in range(row)], axis=0)
        q = qg[(far * 2 + i) * CORES + h, p]
        q = jnp.concatenate([q[:, :HEAD], q[:, HEAD:]], axis=0)
        return _dot(k, q, 1, 1)

    def settle(i, s, room, old):
        if room is not None:
            gap = lax.rem(lax.broadcasted_iota(jnp.int32, (bk, cols), 1), HEAD) - lax.broadcasted_iota(jnp.int32, (bk, cols), 0)
            s = jnp.where(gap >= -room[i], s, HIDDEN)
        top = jnp.maximum(old, s.max(axis=0, keepdims=True))
        s_s[i] = s
        return top, jnp.exp2((old - top) * e)

    def score(i, n, t, room, old):
        return settle(i, raw_score(i, n, t), room, old)

    def weights(i, top):
        return jnp.exp2((s_s[i] - top) * e).astype(jnp.bfloat16)

    def mixed(i, t, w, keep, a):
        v = jnp.concatenate([kvg[t * row + a, HEAD:, :] for a in range(row)], axis=1)
        v = jnp.concatenate([v, jnp.ones((8, bk), jnp.bfloat16)], axis=0)
        mix_s[a, i] = mix_s[a, i] * keep + _dot(v, w)

    def weigh(i, t, top, keep, a):
        mixed(i, t, weights(i, top), keep, a)

    def note(n, parts):
        for i, (top, keep) in enumerate(parts):
            top_s[n, i : i + 1, :] = top
            keep_s[n, i : i + 1, :] = keep

    def noted(ref, n):
        return [ref[n, i : i + 1, :] for i in range(CORES)]

    def room_of(n):
        far, h, _ = of(n)
        return [(place(far * 2 + i)[1] * CORES + h) * HEAD for i in range(2)]

    def both(n, t, m, s, masked):
        tops, keeps, olds = noted(top_s, m), noted(keep_s, m), noted(top_s, n)
        room = room_of(n) if masked else None
        raw = [raw_score(i, n, t) for i in range(CORES)]
        for i in range(CORES):
            weigh(i, s, tops[i], keeps[i], held(m))
        parts = [settle(i, raw[i], room, olds[i]) for i in range(CORES)]
        note(n, parts)

    def sent(n, i):
        far, h, p = of(n)
        return remote(os.at[n, i], og.at[p, u], o_send.at[n, i], o_recv.at[p, u], dev(*place(far * 2 + i), h))

    def finish(n):
        far, h, p = of(n)
        for i in range(2):
            done = (mix_s[held(n), i, :HEAD, :] * (1 / mix_s[held(n), i, HEAD : HEAD + 1, :])).astype(jnp.bfloat16)
            for s in range(2):
                os[n, i, :, s * HEAD : (s + 1) * HEAD] = done[:, s * HEAD : (s + 1) * HEAD].T
        for i in range(2):
            mine = (far * 2 + i) * CORES + h == u
            pl.when(mine)(pltpu.make_async_copy(os.at[n, i], og.at[p, u], o_recv.at[p, u]).start)
            pl.when(jnp.logical_not(mine))(sent(n, i).start)

    def take_q(n):
        far, h, _ = of(n)
        with jax.named_scope("wait_q"):
            for i in range(2):
                at = (far * 2 + i) * CORES + h
                pltpu.make_async_copy(qs.at[0], qg.at[at], q_recv.at[at]).wait()

    top_s[...] = jnp.full(top_s.shape, NEG, jnp.float32)
    mix_s[...] = jnp.zeros(mix_s.shape, jnp.float32)
    zero = jnp.int32(0)
    arrived(1, 1)
    take_q(zero)
    note(zero, [score(i, zero, gx, room_of(zero), old) for i, old in enumerate(noted(top_s, zero))])

    def attend(g, before):
        m, s = before
        start = lax.div(23 - g, 20)
        p, r = lax.div(g + 4, 8) - 1, lax.rem(g + 4, 8)
        k = r - 2 * gx
        per = 4 - gx
        far = lax.div(k + 8, 8)
        j = lax.rem(k + per, per)
        t_a = j + lax.div(j, 2) * (1 - 2 * lax.rem(j, 2))
        t_b = j + (1 - lax.div(j, 2)) * (1 - 2 * j)
        item, t = r + far * (2 + lax.div(k + per, per) - 1 - r), far * (t_a + gx * (t_b - t_a))
        item, t = item + start * (lax.rem(g, 2) - item), t + start * (gx - t)
        far = far * (1 - start)
        p = p + start * (lax.div(g, 2) - p)
        n = p * 4 + item
        own = gx + far * (side - 1 - 2 * gx)

        hooks(g, LATER)

        @pl.when(g == 5 - gx)
        def _():
            for d, i in ((0, 0), (2, 0), (2, 1)):
                arrived(d, i)

        @pl.when(g == 6 + 2 * gx)
        def _():
            arrived(1, 3)

        @pl.when((g == 7) & (gx == 0))
        def _():
            last_gather()

        pl.when(g == 1)(lambda: take_q(zero + 1))
        pl.when(g == 4 + 2 * gx)(lambda: take_q(zero + 2))
        pl.when(g == 8 + gx)(lambda: take_q(zero + 3))

        with jax.named_scope("at"):
            pl.when(t == own)(lambda: both(n, t, m, s, True))
            pl.when(t != own)(lambda: both(n, t, m, s, False))
        pl.when(s == 2 * lax.div(lax.rem(m, 4), 2))(lambda: finish(m))
        return n, t

    def last_gather():
        for d, i in ((0, 2), (2, 2), (2, 3)):
            arrived(d, i)

    at = lax.fori_loop(1, 20, attend, (zero, gx))
    for i in range(CORES):
        weigh(i, at[1], noted(top_s, at[0])[i], noted(keep_s, at[0])[i], held(at[0]))
    finish(at[0])

    for p in range(2):
        with jax.named_scope("wait_o"):
            for k in range(nu):
                pltpu.make_async_copy(os.at[0, 0], og.at[p, k], o_recv.at[p, k]).wait()

        with jax.named_scope("wait_wo"):
            for n in range(slabs):
                load_o(p, n).wait()
        with jax.named_scope("wo"):
            for n in range(slabs):
                more = _dot(og[p, 0], wobuf[p * slabs + n, 0])
                for k in range(1, nu):
                    more += _dot(og[p, k], wobuf[p * slabs + n, k])
                if p == 0:
                    acc[:, n * step : (n + 1) * step] = more + xv[:, n * step : (n + 1) * step].astype(jnp.float32)
                else:
                    y_ref[:, n * step : (n + 1) * step] = (acc[:, n * step : (n + 1) * step] + more).astype(jnp.bfloat16)

    for n in range(nc):
        xx, yy, _ = other(jnp.int32(UNITS[n]))
        for h in range(CORES):
            i = n * CORES + h
            wait = remote(kvs.at[i], kvg.at[me], kv_send.at[i], kv_recv.at[u], dev(xx, yy, h)).wait_send
            if UNITS[n] > 0:
                wait()
            else:
                pl.when(c != h)(wait)
    for i in range(nc):
        for d in range(2):
            passed(d, i).wait_send()
        relayed(i).wait_send()

    def left(n, _):
        xx, yy, cc, _ = target(n)
        pl.when(n < nu - 1)(remote(qs.at[n], qg.at[u], q_send.at[n], q_recv.at[u], dev(xx, yy, cc)).wait_send)
        far, h, _ = of(n)
        for i in range(2):
            pl.when((far * 2 + i) * CORES + h != u)(sent(n, i).wait_send)

    lax.fori_loop(0, nu, left, None)
    pl.when(gx == 1)(last_gather)


def solution(mesh):
    total = mesh.shape["sp"]

    def step(x, gain, wq, wk, wv, wo):
        own, dim = x.shape
        nu = wk.shape[1] // HEAD
        side = math.isqrt(total // CORES)
        group = wq.shape[1] // nu
        half = HEAD // 2
        rate = THETA ** (-jnp.arange(half, dtype=jnp.float32) / half)
        rate = jnp.concatenate([rate, rate])[None]
        any_ = pl.BlockSpec(memory_space=pltpu.HBM)
        vmem = pl.BlockSpec(memory_space=pltpu.VMEM)
        low, wide = jnp.bfloat16, jnp.float32
        dma = pltpu.SemaphoreType.DMA
        cols = 2 * HEAD
        step_o = min(dim, 512)
        y = pl.pallas_call(
            functools.partial(_kernel, side),
            out_shape=jax.ShapeDtypeStruct((own, dim), low),
            in_specs=[any_, vmem, vmem, any_, any_, any_, any_],
            out_specs=vmem,
            scratch_shapes=[
                pltpu.VMEM((own, dim), low),
                pltpu.VMEM((own, dim), low),
                pltpu.VMEM((own, HEAD), wide),
                pltpu.VMEM((own, HEAD), wide),
                pltpu.VMEM((SLOTS, dim, group), low),
                pltpu.VMEM((2 * dim // step_o, nu, cols, step_o), low),
                pltpu.VMEM((nu, 2 * HEAD, own), low),
                pltpu.VMEM((total, 2 * HEAD, own), low),
                pltpu.VMEM((nu, 2, own, cols), low),
                pltpu.VMEM((nu, 2, own, cols), low),
                pltpu.VMEM((nu, CORES, own, cols), low),
                pltpu.VMEM((2, nu, own, cols), low),
                pltpu.VMEM((own, dim), wide),
                pltpu.VMEM((nu, CORES, cols), wide),
                pltpu.VMEM((nu, CORES, cols), wide),
                pltpu.VMEM((5, CORES, HEAD + 8, cols), wide),
                pltpu.VMEM((CORES, side * CORES * own, cols), wide),
                dma, dma((SLOTS, 2)), dma((2 * dim // step_o,)),
                dma((nu,)), dma((nu,)), dma((3, 4)), dma((3, 4)),
                dma((nu,)), dma((nu,)), dma((nu, CORES)), dma((2, nu)),
            ],
            compiler_params=pltpu.CompilerParams(collective_id=0, has_side_effects=True, vmem_limit_bytes=VMEM),
        )(x, gain.reshape(-1, HEAD), rate, wq, wk, wv, wo.reshape(nu, 2, cols, dim))
        return y

    tokens, whole = P(("dp", "sp"), None), P(None, None)
    return jax.shard_map(
        step,
        mesh=mesh,
        in_specs=(tokens, P(None), whole, whole, whole, whole),
        out_specs=tokens,
        check_vma=False,
    )
```

```python
import functools
import math

import jax
import jax.numpy as jnp
from jax import lax
from jax.experimental import pallas as pl
from jax.experimental.pallas import tpu as pltpu
from jax.sharding import PartitionSpec as P

HEAD = 128
THETA = 10000
CORES = 2
NEG = -1e30
HIDDEN = 2 * NEG
LOG2E = 1.4426950408889634
SLOTS = 3
MESH = pl.DeviceIdType.MESH
VMEM = 63 * 2**20
UNITS = [1, 2, 0, 3]
HOOKS = [
    {2: [("pass", 2)], 4: [("relay", 0)], 6: [("relay", 2)], 7: [("pass", 3)], 8: [("pass", 1)]},
    {2: [("pass", 1)], 3: [("pass", 3)], 6: [("relay", 1)], 8: [("relay", 3), ("pass", 2)]},
]
LATER = [{3: [("relay", 3)], 5: [("relay", 1)]}, {2: [("relay", 0)], 5: [("relay", 2)]}]


def _dot(a, b, ca=1, cb=0):
    return lax.dot_general(a, b, (((ca,), (cb,)), ((), ())), preferred_element_type=jnp.float32)


def _kernel(side, x_hbm, gain_ref, rate_ref, wq, wk, wv, wo, y_ref,
            xv, av, cos_ref, sin_ref, wbuf, wobuf, kvs, kvg, qs, qg, os, og, acc, top_s, keep_s, mix_s, s_s,
            x_sem, w_sem, wo_sem, kv_send, kv_recv, g_send, g_recv, q_send, q_recv, o_send, o_recv):
    own, dim = xv.shape
    nc = 4
    nu = nc * CORES
    cols = 2 * HEAD
    group = 2 * cols
    me = lax.axis_index("sp")
    x, y, c = lax.div(me, CORES * side), lax.rem(lax.div(me, CORES), side), lax.rem(me, CORES)
    hx, hy = lax.div(x, 2), lax.div(y, 2)
    gx, gy = lax.rem(x + hx, 2), lax.rem(y + hy, 2)
    u = (hx * 2 + hy) * CORES + c

    def flip(a, d, top=1):
        return a + d * (top - 2 * a)

    def dev(xx, yy, cc):
        return {"sp": (xx * side + yy) * CORES + cc}

    def remote(src, dst, send, recv, to):
        return pltpu.make_async_remote_copy(src_ref=src, dst_ref=dst, send_sem=send, recv_sem=recv, device_id=to, device_id_type=MESH)

    def other(n):
        dx, dy = lax.rem(n, 2), lax.rem(lax.div(n + 1, 2), 2)
        return flip(x, dx, side - 1), flip(y, dy, side - 1), flip(hx, dx) * 2 + flip(hy, dy)

    def place(i, fx=0, fy=0):
        ax, ay = flip(gx, fx), flip(gy, fy)
        return flip(ax, i // 2, side - 1), flip(ay, i % 2, side - 1)

    def beside(a):
        return a + 1 - 2 * lax.rem(a, 2)

    def load_kv(n):
        _, _, chip = other(jnp.int32(UNITS[n]))
        wide = CORES * HEAD
        at = pl.ds(pl.multiple_of(chip * wide, wide), wide)
        return [pltpu.make_async_copy(wk.at[:, at], wbuf.at[n % SLOTS, :, pl.ds(0, wide)], w_sem.at[n % SLOTS, 0]),
                pltpu.make_async_copy(wv.at[:, at], wbuf.at[n % SLOTS, :, pl.ds(wide, wide)], w_sem.at[n % SLOTS, 1])]

    def target(j):
        xx, yy, chip = other(lax.rem(lax.div(j, CORES) + 1, nc))
        cc = flip(c, 1 - lax.rem(j, CORES))
        return xx, yy, cc, chip * CORES + cc

    def load_q(j):
        at = pl.ds(pl.multiple_of(target(j)[3] * group, group), group)
        slot = lax.rem(j + nc, SLOTS)
        return pltpu.make_async_copy(wq.at[:, at], wbuf.at[slot], w_sem.at[slot, 0])

    step = wobuf.shape[3]
    slabs = dim // step

    def load_o(p, n):
        at = pl.ds(pl.multiple_of(n * step, step), step)
        return pltpu.make_async_copy(wo.at[:, p, :, at], wobuf.at[p * slabs + n], wo_sem.at[p * slabs + n])

    get_x = pltpu.make_async_copy(x_hbm, xv, x_sem)
    get_x.start()
    for copy in load_kv(0):
        copy.start()

    barrier = pltpu.get_barrier_semaphore()
    peers = [dev(flip(x, dx, side - 1), flip(y, dy, side - 1), flip(c, dc)) for dx in range(2) for dy in range(2) for dc in range(2) if dx + dy + dc]
    near = [(beside(x), y), (x, beside(y))]
    peers += [dev(xx, yy, c) for xx, yy in near]
    for peer in peers:
        pl.semaphore_signal(barrier, inc=1, device_id=peer, device_id_type=MESH)

    place_ = (me * own + lax.broadcasted_iota(jnp.int32, (own, HEAD), 0)).astype(jnp.float32)
    angle = place_ * rate_ref[...]
    second = lax.broadcasted_iota(jnp.int32, (own, HEAD), 1) >= HEAD // 2
    cos_ref[...] = jnp.cos(angle)
    sin_ref[...] = jnp.where(second, jnp.sin(angle), -jnp.sin(angle))
    for n in range(1, SLOTS):
        for copy in load_kv(n):
            copy.start()
    with jax.named_scope("wait_x"):
        get_x.wait()
    wide = xv[...].astype(jnp.float32)
    scale = lax.rsqrt(jnp.mean(wide * wide, -1, keepdims=True) + 1e-6)
    lanes = gain_ref.shape[1]
    for k in range(dim // lanes):
        at = slice(k * lanes, (k + 1) * lanes)
        av[:, at] = (xv[:, at].astype(jnp.float32) * scale * gain_ref[k : k + 1, :].astype(jnp.float32)).astype(jnp.bfloat16)
    with jax.named_scope("wait_b"):
        pl.semaphore_wait(barrier, len(peers))

    def turn(t):
        t = t.astype(jnp.float32)
        return (t * cos_ref[...] + pltpu.roll(t, HEAD // 2, 1) * sin_ref[...]).astype(jnp.bfloat16)

    def chip_block(xx, yy):
        return kvg.at[pl.ds((xx * side + yy) * CORES, CORES)]

    def passed(d, i):
        block = chip_block(*place(i))
        return remote(block, block, g_send.at[d, i], g_recv.at[d, i], dev(*near[d], c))

    def relayed(i):
        odd = lax.rem(i, 2)
        block = chip_block(*place(i, odd, 1 - odd))
        (ax, ay), (bx, by) = near
        return remote(block, block, g_send.at[2, i], g_recv.at[2, i], dev(ax + odd * (bx - ax), ay + odd * (by - ay), c))

    def arrived(d, i):
        with jax.named_scope("wait_kvg"):
            block = chip_block(*place(i, int(d != 1), int(d != 0)))
            pltpu.make_async_copy(block, block, g_recv.at[d, i]).wait()

    def relay(i):
        odd = lax.rem(i, 2)
        with jax.named_scope("wait_relay"):
            block = chip_block(*place(i, odd, 1 - odd))
            pltpu.make_async_copy(block, block, g_recv.at[1 - odd, i]).wait()
        relayed(i).start()

    def pass_on(i):
        with jax.named_scope("wait_kvx"):
            for h in range(CORES):
                pltpu.make_async_copy(kvs.at[0], kvg.at[dev(*place(i), h)["sp"]], kv_recv.at[i * CORES + h]).wait()
        for d in range(2):
            passed(d, i).start()

    def turn_to(n):
        _, _, chip = other(jnp.int32(n))
        return chip

    for n in range(nc):
        with jax.named_scope("wait_wkv"):
            for copy in load_kv(n):
                copy.wait()
        both = _dot(av[...], wbuf[n % SLOTS]).astype(jnp.bfloat16)
        if n + SLOTS < nc:
            for copy in load_kv(n + SLOTS):
                copy.start()
        else:
            load_q(jnp.int32(n + SLOTS - nc)).start()
        xx, yy, _ = other(jnp.int32(UNITS[n]))
        for h in range(CORES):
            i = n * CORES + h
            kvs[i, :HEAD, :] = turn(both[:, h * HEAD : (h + 1) * HEAD])
            at = (CORES + h) * HEAD
            kvs[i, HEAD:, :] = both[:, at : at + HEAD].T
            there = remote(kvs.at[i], kvg.at[me], kv_send.at[i], kv_recv.at[u], dev(xx, yy, h))
            if UNITS[n] > 0:
                there.start()
            else:
                here = pltpu.make_async_copy(kvs.at[i], kvg.at[me], kv_recv.at[u])
                pl.when(c == h)(here.start)
                pl.when(c != h)(there.start)
        if n == 3:
            pass_on(turn_to(0))

    def hooks(j, table):
        for half in range(2):
            for at, do in table[half].items():
                if isinstance(j, int) and j != at:
                    continue
                for kind, i in do:
                    act = functools.partial(pass_on if kind == "pass" else relay, turn_to(i))
                    pl.when((j == at) & (hx == half))(act)

    def queries(j, _):
        with jax.named_scope("wait_wq"):
            load_q(j).wait()
        slot = lax.rem(j + nc, SLOTS)
        t = _dot(av[...], wbuf[slot]).astype(jnp.bfloat16)

        @pl.when(j + SLOTS < nu)
        def _():
            load_q(j + SLOTS).start()

        @pl.when(j + SLOTS >= nu)
        def _():
            load_o(0, j + SLOTS - nu).start()

        for p in range(2):
            for s in range(2):
                at = p * cols + s * HEAD
                qs[j, p, :, s * HEAD : (s + 1) * HEAD] = turn(t[:, at : at + HEAD])
        xx, yy, cc, _ = target(j)
        here = pltpu.make_async_copy(qs.at[j], qg.at[u], q_recv.at[u])
        there = remote(qs.at[j], qg.at[u], q_send.at[j], q_recv.at[u], dev(xx, yy, cc))
        pl.when(j == nu - 1)(here.start)
        pl.when(j < nu - 1)(there.start)

        hooks(j, HOOKS)

    lax.fori_loop(0, nu, queries, None)
    hooks(nu, HOOKS)
    for n in range(SLOTS, slabs):
        load_o(0, n).start()
    for n in range(slabs):
        load_o(1, n).start()

    e = HEAD**-0.5 * LOG2E
    row = side * CORES
    bk = row * HEAD

    def of(n):
        return lax.rem(lax.div(n, 2), 2), lax.rem(n, 2), lax.div(n, 4)

    def held(n):
        far, h, p = of(n)
        return (1 - far) * (h + 2 * p) + 4 * far

    def raw_score(i, n, t):
        far, h, p = of(n)
        k = jnp.concatenate([kvg[t * row + a, :HEAD, :] for a in range(row)], axis=0)
        q = qg[(far * 2 + i) * CORES + h, p]
        q = jnp.concatenate([q[:, :HEAD], q[:, HEAD:]], axis=0)
        return _dot(k, q, 1, 1)

    def settle(i, s, room, old):
        if room is not None:
            gap = lax.rem(lax.broadcasted_iota(jnp.int32, (bk, cols), 1), HEAD) - lax.broadcasted_iota(jnp.int32, (bk, cols), 0)
            s = jnp.where(gap >= -room[i], s, HIDDEN)
        top = jnp.maximum(old, s.max(axis=0, keepdims=True))
        s_s[i] = s
        return top, jnp.exp2((old - top) * e)

    def score(i, n, t, room, old):
        return settle(i, raw_score(i, n, t), room, old)

    def weights(i, top):
        return jnp.exp2((s_s[i] - top) * e).astype(jnp.bfloat16)

    def mixed(i, t, w, keep, a):
        v = jnp.concatenate([kvg[t * row + a, HEAD:, :] for a in range(row)], axis=1)
        v = jnp.concatenate([v, jnp.ones((8, bk), jnp.bfloat16)], axis=0)
        mix_s[a, i] = mix_s[a, i] * keep + _dot(v, w)

    def weigh(i, t, top, keep, a):
        mixed(i, t, weights(i, top), keep, a)

    def note(n, parts):
        for i, (top, keep) in enumerate(parts):
            top_s[n, i : i + 1, :] = top
            keep_s[n, i : i + 1, :] = keep

    def noted(ref, n):
        return [ref[n, i : i + 1, :] for i in range(CORES)]

    def room_of(n):
        far, h, _ = of(n)
        return [(place(far * 2 + i)[1] * CORES + h) * HEAD for i in range(2)]

    def both(n, t, m, s, masked):
        tops, keeps, olds = noted(top_s, m), noted(keep_s, m), noted(top_s, n)
        room = room_of(n) if masked else None
        raw = [raw_score(i, n, t) for i in range(CORES)]
        for i in range(CORES):
            weigh(i, s, tops[i], keeps[i], held(m))
        parts = [settle(i, raw[i], room, olds[i]) for i in range(CORES)]
        note(n, parts)

    def sent(n, i):
        far, h, p = of(n)
        return remote(os.at[n, i], og.at[p, u], o_send.at[n, i], o_recv.at[p, u], dev(*place(far * 2 + i), h))

    def finish(n):
        far, h, p = of(n)
        for i in range(2):
            done = (mix_s[held(n), i, :HEAD, :] * (1 / mix_s[held(n), i, HEAD : HEAD + 1, :])).astype(jnp.bfloat16)
            for s in range(2):
                os[n, i, :, s * HEAD : (s + 1) * HEAD] = done[:, s * HEAD : (s + 1) * HEAD].T
        for i in range(2):
            mine = (far * 2 + i) * CORES + h == u
            pl.when(mine)(pltpu.make_async_copy(os.at[n, i], og.at[p, u], o_recv.at[p, u]).start)
            pl.when(jnp.logical_not(mine))(sent(n, i).start)

    def take_q(n):
        far, h, _ = of(n)
        with jax.named_scope("wait_q"):
            for i in range(2):
                at = (far * 2 + i) * CORES + h
                pltpu.make_async_copy(qs.at[0], qg.at[at], q_recv.at[at]).wait()

    top_s[...] = jnp.full(top_s.shape, NEG, jnp.float32)
    mix_s[...] = jnp.zeros(mix_s.shape, jnp.float32)
    zero = jnp.int32(0)
    arrived(1, 1)
    take_q(zero)
    note(zero, [score(i, zero, gx, room_of(zero), old) for i, old in enumerate(noted(top_s, zero))])

    def attend(g, before):
        m, s = before
        start = lax.div(23 - g, 20)
        p, r = lax.div(g + 4, 8) - 1, lax.rem(g + 4, 8)
        k = r - 2 * gx
        per = 4 - gx
        far = lax.div(k + 8, 8)
        j = lax.rem(k + per, per)
        t_a = j + lax.div(j, 2) * (1 - 2 * lax.rem(j, 2))
        t_b = j + (1 - lax.div(j, 2)) * (1 - 2 * j)
        item, t = r + far * (2 + lax.div(k + per, per) - 1 - r), far * (t_a + gx * (t_b - t_a))
        item, t = item + start * (lax.rem(g, 2) - item), t + start * (gx - t)
        far = far * (1 - start)
        p = p + start * (lax.div(g, 2) - p)
        n = p * 4 + item
        own = gx + far * (side - 1 - 2 * gx)

        hooks(g, LATER)

        @pl.when(g == 5 - gx)
        def _():
            for d, i in ((0, 0), (2, 0), (2, 1)):
                arrived(d, i)

        @pl.when(g == 6 + 2 * gx)
        def _():
            arrived(1, 3)

        @pl.when((g == 7) & (gx == 0))
        def _():
            last_gather()

        pl.when(g == 1)(lambda: take_q(zero + 1))
        pl.when(g == 4 + 2 * gx)(lambda: take_q(zero + 2))
        pl.when(g == 8 + gx)(lambda: take_q(zero + 3))

        with jax.named_scope("at"):
            pl.when(t == own)(lambda: both(n, t, m, s, True))
            pl.when(t != own)(lambda: both(n, t, m, s, False))
        pl.when(s == 2 * lax.div(lax.rem(m, 4), 2))(lambda: finish(m))
        return n, t

    def last_gather():
        for d, i in ((0, 2), (2, 2), (2, 3)):
            arrived(d, i)

    at = lax.fori_loop(1, 20, attend, (zero, gx))
    for i in range(CORES):
        weigh(i, at[1], noted(top_s, at[0])[i], noted(keep_s, at[0])[i], held(at[0]))
    finish(at[0])

    for p in range(2):
        with jax.named_scope("wait_o"):
            for k in range(nu):
                pltpu.make_async_copy(os.at[0, 0], og.at[p, k], o_recv.at[p, k]).wait()

        with jax.named_scope("wait_wo"):
            for n in range(slabs):
                load_o(p, n).wait()
        with jax.named_scope("wo"):
            for n in range(slabs):
                more = _dot(og[p, 0], wobuf[p * slabs + n, 0])
                for k in range(1, nu):
                    more += _dot(og[p, k], wobuf[p * slabs + n, k])
                if p == 0:
                    acc[:, n * step : (n + 1) * step] = more + xv[:, n * step : (n + 1) * step].astype(jnp.float32)
                else:
                    y_ref[:, n * step : (n + 1) * step] = (acc[:, n * step : (n + 1) * step] + more).astype(jnp.bfloat16)

    for n in range(nc):
        xx, yy, _ = other(jnp.int32(UNITS[n]))
        for h in range(CORES):
            i = n * CORES + h
            wait = remote(kvs.at[i], kvg.at[me], kv_send.at[i], kv_recv.at[u], dev(xx, yy, h)).wait_send
            if UNITS[n] > 0:
                wait()
            else:
                pl.when(c != h)(wait)
    for i in range(nc):
        for d in range(2):
            passed(d, i).wait_send()
        relayed(i).wait_send()

    def left(n, _):
        xx, yy, cc, _ = target(n)
        pl.when(n < nu - 1)(remote(qs.at[n], qg.at[u], q_send.at[n], q_recv.at[u], dev(xx, yy, cc)).wait_send)
        far, h, _ = of(n)
        for i in range(2):
            pl.when((far * 2 + i) * CORES + h != u)(sent(n, i).wait_send)

    lax.fori_loop(0, nu, left, None)
    pl.when(gx == 1)(last_gather)


def solution(mesh):
    total = mesh.shape["sp"]

    def step(x, gain, wq, wk, wv, wo):
        own, dim = x.shape
        nu = wk.shape[1] // HEAD
        side = math.isqrt(total // CORES)
        group = wq.shape[1] // nu
        half = HEAD // 2
        rate = THETA ** (-jnp.arange(half, dtype=jnp.float32) / half)
        rate = jnp.concatenate([rate, rate])[None]
        any_ = pl.BlockSpec(memory_space=pltpu.HBM)
        vmem = pl.BlockSpec(memory_space=pltpu.VMEM)
        low, wide = jnp.bfloat16, jnp.float32
        dma = pltpu.SemaphoreType.DMA
        cols = 2 * HEAD
        step_o = min(dim, 512)
        y = pl.pallas_call(
            functools.partial(_kernel, side),
            out_shape=jax.ShapeDtypeStruct((own, dim), low),
            in_specs=[any_, vmem, vmem, any_, any_, any_, any_],
            out_specs=vmem,
            scratch_shapes=[
                pltpu.VMEM((own, dim), low),
                pltpu.VMEM((own, dim), low),
                pltpu.VMEM((own, HEAD), wide),
                pltpu.VMEM((own, HEAD), wide),
                pltpu.VMEM((SLOTS, dim, group), low),
                pltpu.VMEM((2 * dim // step_o, nu, cols, step_o), low),
                pltpu.VMEM((nu, 2 * HEAD, own), low),
                pltpu.VMEM((total, 2 * HEAD, own), low),
                pltpu.VMEM((nu, 2, own, cols), low),
                pltpu.VMEM((nu, 2, own, cols), low),
                pltpu.VMEM((nu, CORES, own, cols), low),
                pltpu.VMEM((2, nu, own, cols), low),
                pltpu.VMEM((own, dim), wide),
                pltpu.VMEM((nu, CORES, cols), wide),
                pltpu.VMEM((nu, CORES, cols), wide),
                pltpu.VMEM((5, CORES, HEAD + 8, cols), wide),
                pltpu.VMEM((CORES, side * CORES * own, cols), wide),
                dma, dma((SLOTS, 2)), dma((2 * dim // step_o,)),
                dma((nu,)), dma((nu,)), dma((3, 4)), dma((3, 4)),
                dma((nu,)), dma((nu,)), dma((nu, CORES)), dma((2, nu)),
            ],
            compiler_params=pltpu.CompilerParams(collective_id=0, has_side_effects=True, vmem_limit_bytes=VMEM),
        )(x, gain.reshape(-1, HEAD), rate, wq, wk, wv, wo.reshape(nu, 2, cols, dim))
        return y

    tokens, whole = P(("dp", "sp"), None), P(None, None)
    return jax.shard_map(
        step,
        mesh=mesh,
        in_specs=(tokens, P(None), whole, whole, whole, whole),
        out_specs=tokens,
        check_vma=False,
    )
```

```python
import functools
import math

import jax
import jax.numpy as jnp
from jax import lax
from jax.experimental import pallas as pl
from jax.experimental.pallas import tpu as pltpu
from jax.sharding import PartitionSpec as P

HEAD = 128
THETA = 10000
CORES = 2
NEG = -1e30
HIDDEN = 2 * NEG
LOG2E = 1.4426950408889634
SLOTS = 3
MESH = pl.DeviceIdType.MESH
VMEM = 63 * 2**20
UNITS = [1, 2, 0, 3]
HOOKS = [
    {2: [("pass", 2)], 4: [("relay", 0)], 6: [("relay", 2)], 7: [("pass", 3)], 8: [("pass", 1)]},
    {2: [("pass", 1)], 3: [("pass", 3)], 6: [("relay", 1)], 8: [("relay", 3), ("pass", 2)]},
]
LATER = [{3: [("relay", 3)], 5: [("relay", 1)]}, {2: [("relay", 0)], 5: [("relay", 2)]}]


def _dot(a, b, ca=1, cb=0):
    return lax.dot_general(a, b, (((ca,), (cb,)), ((), ())), preferred_element_type=jnp.float32)


def _kernel(side, x_hbm, gain_ref, rate_ref, wq, wk, wv, wo, y_ref,
            xv, av, cos_ref, sin_ref, wbuf, wobuf, kvs, kvg, qs, qg, os, og, acc, top_s, keep_s, mix_s, s_s,
            x_sem, w_sem, wo_sem, kv_send, kv_recv, g_send, g_recv, q_send, q_recv, o_send, o_recv):
    own, dim = xv.shape
    nc = 4
    nu = nc * CORES
    cols = 2 * HEAD
    group = 2 * cols
    me = lax.axis_index("sp")
    x, y, c = lax.div(me, CORES * side), lax.rem(lax.div(me, CORES), side), lax.rem(me, CORES)
    hx, hy = lax.div(x, 2), lax.div(y, 2)
    gx, gy = lax.rem(x + hx, 2), lax.rem(y + hy, 2)
    u = (hx * 2 + hy) * CORES + c

    def flip(a, d, top=1):
        return a + d * (top - 2 * a)

    def dev(xx, yy, cc):
        return {"sp": (xx * side + yy) * CORES + cc}

    def remote(src, dst, send, recv, to):
        return pltpu.make_async_remote_copy(src_ref=src, dst_ref=dst, send_sem=send, recv_sem=recv, device_id=to, device_id_type=MESH)

    def other(n):
        dx, dy = lax.rem(n, 2), lax.rem(lax.div(n + 1, 2), 2)
        return flip(x, dx, side - 1), flip(y, dy, side - 1), flip(hx, dx) * 2 + flip(hy, dy)

    def place(i, fx=0, fy=0):
        ax, ay = flip(gx, fx), flip(gy, fy)
        return flip(ax, i // 2, side - 1), flip(ay, i % 2, side - 1)

    def beside(a):
        return a + 1 - 2 * lax.rem(a, 2)

    def load_kv(n):
        _, _, chip = other(jnp.int32(UNITS[n]))
        wide = CORES * HEAD
        at = pl.ds(pl.multiple_of(chip * wide, wide), wide)
        return [pltpu.make_async_copy(wk.at[:, at], wbuf.at[n % SLOTS, :, pl.ds(0, wide)], w_sem.at[n % SLOTS, 0]),
                pltpu.make_async_copy(wv.at[:, at], wbuf.at[n % SLOTS, :, pl.ds(wide, wide)], w_sem.at[n % SLOTS, 1])]

    def target(j):
        return *other(lax.rem(j + 1, nc)), lax.div(j, nc)

    def load_q(j):
        _, _, chip, p = target(j)
        slot = lax.rem(j + nc, SLOTS)
        copies = []
        for h in range(CORES):
            at = pl.ds(pl.multiple_of((chip * CORES + h) * group + p * cols, cols), cols)
            copies.append(pltpu.make_async_copy(wq.at[:, at], wbuf.at[slot, :, pl.ds(h * cols, cols)], w_sem.at[slot, h]))
        return copies

    def send_q(j, h):
        xx, yy, _, p = target(j)
        return remote(qs.at[j, h], qg.at[p, u], q_send.at[j, h], q_recv.at[p, u], dev(xx, yy, h))

    def stays(j, h):
        return (lax.rem(j, nc) == nc - 1) & (c == h)

    step = wobuf.shape[3]
    slabs = dim // step

    def load_o(p, n):
        at = pl.ds(pl.multiple_of(n * step, step), step)
        return pltpu.make_async_copy(wo.at[:, p, :, at], wobuf.at[p * slabs + n], wo_sem.at[p * slabs + n])

    get_x = pltpu.make_async_copy(x_hbm, xv, x_sem)
    get_x.start()
    for copy in load_kv(0):
        copy.start()

    barrier = pltpu.get_barrier_semaphore()
    peers = [dev(flip(x, dx, side - 1), flip(y, dy, side - 1), flip(c, dc)) for dx in range(2) for dy in range(2) for dc in range(2) if dx + dy + dc]
    near = [(beside(x), y), (x, beside(y))]
    peers += [dev(xx, yy, c) for xx, yy in near]
    for peer in peers:
        pl.semaphore_signal(barrier, inc=1, device_id=peer, device_id_type=MESH)

    place_ = (me * own + lax.broadcasted_iota(jnp.int32, (own, HEAD), 0)).astype(jnp.float32)
    angle = place_ * rate_ref[...]
    second = lax.broadcasted_iota(jnp.int32, (own, HEAD), 1) >= HEAD // 2
    cos_ref[...] = jnp.cos(angle)
    sin_ref[...] = jnp.where(second, jnp.sin(angle), -jnp.sin(angle))
    for n in range(1, SLOTS):
        for copy in load_kv(n):
            copy.start()
    with jax.named_scope("wait_x"):
        get_x.wait()
    wide = xv[...].astype(jnp.float32)
    scale = lax.rsqrt(jnp.mean(wide * wide, -1, keepdims=True) + 1e-6)
    lanes = gain_ref.shape[1]
    for k in range(dim // lanes):
        at = slice(k * lanes, (k + 1) * lanes)
        av[:, at] = (xv[:, at].astype(jnp.float32) * scale * gain_ref[k : k + 1, :].astype(jnp.float32)).astype(jnp.bfloat16)
    with jax.named_scope("wait_b"):
        pl.semaphore_wait(barrier, len(peers))

    def turn(t):
        t = t.astype(jnp.float32)
        return (t * cos_ref[...] + pltpu.roll(t, HEAD // 2, 1) * sin_ref[...]).astype(jnp.bfloat16)

    def chip_block(xx, yy):
        return kvg.at[pl.ds((xx * side + yy) * CORES, CORES)]

    def passed(d, i):
        block = chip_block(*place(i))
        return remote(block, block, g_send.at[d, i], g_recv.at[d, i], dev(*near[d], c))

    def relayed(i):
        odd = lax.rem(i, 2)
        block = chip_block(*place(i, odd, 1 - odd))
        (ax, ay), (bx, by) = near
        return remote(block, block, g_send.at[2, i], g_recv.at[2, i], dev(ax + odd * (bx - ax), ay + odd * (by - ay), c))

    def arrived(d, i):
        with jax.named_scope("wait_kvg"):
            block = chip_block(*place(i, int(d != 1), int(d != 0)))
            pltpu.make_async_copy(block, block, g_recv.at[d, i]).wait()

    def relay(i):
        odd = lax.rem(i, 2)
        with jax.named_scope("wait_relay"):
            block = chip_block(*place(i, odd, 1 - odd))
            pltpu.make_async_copy(block, block, g_recv.at[1 - odd, i]).wait()
        relayed(i).start()

    def pass_on(i):
        with jax.named_scope("wait_kvx"):
            for h in range(CORES):
                pltpu.make_async_copy(kvs.at[0], kvg.at[dev(*place(i), h)["sp"]], kv_recv.at[i * CORES + h]).wait()
        for d in range(2):
            passed(d, i).start()

    def turn_to(n):
        _, _, chip = other(jnp.int32(n))
        return chip

    for n in range(nc):
        with jax.named_scope("wait_wkv"):
            for copy in load_kv(n):
                copy.wait()
        both = _dot(av[...], wbuf[n % SLOTS]).astype(jnp.bfloat16)
        if n + SLOTS < nc:
            for copy in load_kv(n + SLOTS):
                copy.start()
        else:
            for copy in load_q(jnp.int32(n + SLOTS - nc)):
                copy.start()
        xx, yy, _ = other(jnp.int32(UNITS[n]))
        for h in range(CORES):
            i = n * CORES + h
            kvs[i, :HEAD, :] = turn(both[:, h * HEAD : (h + 1) * HEAD])
            at = (CORES + h) * HEAD
            kvs[i, HEAD:, :] = both[:, at : at + HEAD].T
            there = remote(kvs.at[i], kvg.at[me], kv_send.at[i], kv_recv.at[u], dev(xx, yy, h))
            if UNITS[n] > 0:
                there.start()
            else:
                here = pltpu.make_async_copy(kvs.at[i], kvg.at[me], kv_recv.at[u])
                pl.when(c == h)(here.start)
                pl.when(c != h)(there.start)
        if n == 3:
            pass_on(turn_to(0))

    def hooks(j, table):
        for half in range(2):
            for at, do in table[half].items():
                if isinstance(j, int) and j != at:
                    continue
                for kind, i in do:
                    act = functools.partial(pass_on if kind == "pass" else relay, turn_to(i))
                    pl.when((j == at) & (hx == half))(act)

    def queries(j, _):
        with jax.named_scope("wait_wq"):
            for copy in load_q(j):
                copy.wait()
        slot = lax.rem(j + nc, SLOTS)
        t = _dot(av[...], wbuf[slot]).astype(jnp.bfloat16)

        @pl.when(j + SLOTS < nu)
        def _():
            for copy in load_q(j + SLOTS):
                copy.start()

        @pl.when(j + SLOTS >= nu)
        def _():
            load_o(0, j + SLOTS - nu).start()

        for h in range(CORES):
            for s in range(2):
                at = h * cols + s * HEAD
                qs[j, h, :, s * HEAD : (s + 1) * HEAD] = turn(t[:, at : at + HEAD])
        p = target(j)[3]
        for h in range(CORES):
            pl.when(stays(j, h))(pltpu.make_async_copy(qs.at[j, h], qg.at[p, u], q_recv.at[p, u]).start)
            pl.when(jnp.logical_not(stays(j, h)))(send_q(j, h).start)

        hooks(j, HOOKS)

    lax.fori_loop(0, nu, queries, None)
    hooks(nu, HOOKS)
    for n in range(SLOTS, slabs):
        load_o(0, n).start()
    for n in range(slabs):
        load_o(1, n).start()

    e = HEAD**-0.5 * LOG2E
    row = side * CORES
    bk = row * HEAD

    def of(n):
        return lax.rem(lax.div(n, 2), 2), lax.rem(n, 2), lax.div(n, 4)

    def held(n):
        far, h, p = of(n)
        return (1 - far) * (h + 2 * p) + 4 * far

    def raw_score(i, n, t):
        far, h, p = of(n)
        k = jnp.concatenate([kvg[t * row + a, :HEAD, :] for a in range(row)], axis=0)
        q = qg[p, (far * 2 + i) * CORES + h]
        q = jnp.concatenate([q[:, :HEAD], q[:, HEAD:]], axis=0)
        return _dot(k, q, 1, 1)

    def settle(i, s, room, old):
        if room is not None:
            gap = lax.rem(lax.broadcasted_iota(jnp.int32, (bk, cols), 1), HEAD) - lax.broadcasted_iota(jnp.int32, (bk, cols), 0)
            s = jnp.where(gap >= -room[i], s, HIDDEN)
        top = jnp.maximum(old, s.max(axis=0, keepdims=True))
        s_s[i] = s
        return top, jnp.exp2((old - top) * e)

    def score(i, n, t, room, old):
        return settle(i, raw_score(i, n, t), room, old)

    def weights(i, top):
        return jnp.exp2((s_s[i] - top) * e).astype(jnp.bfloat16)

    def mixed(i, t, w, keep, a):
        v = jnp.concatenate([kvg[t * row + a, HEAD:, :] for a in range(row)], axis=1)
        v = jnp.concatenate([v, jnp.ones((8, bk), jnp.bfloat16)], axis=0)
        mix_s[a, i] = mix_s[a, i] * keep + _dot(v, w)

    def weigh(i, t, top, keep, a):
        mixed(i, t, weights(i, top), keep, a)

    def note(n, parts):
        for i, (top, keep) in enumerate(parts):
            top_s[n, i : i + 1, :] = top
            keep_s[n, i : i + 1, :] = keep

    def noted(ref, n):
        return [ref[n, i : i + 1, :] for i in range(CORES)]

    def room_of(n):
        far, h, _ = of(n)
        return [(place(far * 2 + i)[1] * CORES + h) * HEAD for i in range(2)]

    def both(n, t, m, s, masked):
        tops, keeps, olds = noted(top_s, m), noted(keep_s, m), noted(top_s, n)
        room = room_of(n) if masked else None
        raw = [raw_score(i, n, t) for i in range(CORES)]
        for i in range(CORES):
            weigh(i, s, tops[i], keeps[i], held(m))
        parts = [settle(i, raw[i], room, olds[i]) for i in range(CORES)]
        note(n, parts)

    def sent(n, i):
        far, h, p = of(n)
        return remote(os.at[n, i], og.at[p, u], o_send.at[n, i], o_recv.at[p, u], dev(*place(far * 2 + i), h))

    def finish(n):
        far, h, p = of(n)
        for i in range(2):
            done = (mix_s[held(n), i, :HEAD, :] * (1 / mix_s[held(n), i, HEAD : HEAD + 1, :])).astype(jnp.bfloat16)
            for s in range(2):
                os[n, i, :, s * HEAD : (s + 1) * HEAD] = done[:, s * HEAD : (s + 1) * HEAD].T
        for i in range(2):
            mine = (far * 2 + i) * CORES + h == u
            pl.when(mine)(pltpu.make_async_copy(os.at[n, i], og.at[p, u], o_recv.at[p, u]).start)
            pl.when(jnp.logical_not(mine))(sent(n, i).start)

    def take_q(n):
        far, h, p = of(n)
        with jax.named_scope("wait_q"):
            for i in range(2):
                at = (far * 2 + i) * CORES + h
                pltpu.make_async_copy(qs.at[0, 0], qg.at[p, at], q_recv.at[p, at]).wait()

    top_s[...] = jnp.full(top_s.shape, NEG, jnp.float32)
    mix_s[...] = jnp.zeros(mix_s.shape, jnp.float32)
    zero = jnp.int32(0)
    arrived(1, 1)
    take_q(zero)
    note(zero, [score(i, zero, gx, room_of(zero), old) for i, old in enumerate(noted(top_s, zero))])

    def attend(g, before):
        m, s = before
        start = lax.div(23 - g, 20)
        p, r = lax.div(g + 4, 8) - 1, lax.rem(g + 4, 8)
        k = r - 2 * gx
        per = 4 - gx
        far = lax.div(k + 8, 8)
        j = lax.rem(k + per, per)
        t_a = j + lax.div(j, 2) * (1 - 2 * lax.rem(j, 2))
        t_b = j + (1 - lax.div(j, 2)) * (1 - 2 * j)
        item, t = r + far * (2 + lax.div(k + per, per) - 1 - r), far * (t_a + gx * (t_b - t_a))
        item, t = item + start * (lax.rem(g, 2) - item), t + start * (gx - t)
        far = far * (1 - start)
        p = p + start * (lax.div(g, 2) - p)
        n = p * 4 + item
        own = gx + far * (side - 1 - 2 * gx)

        hooks(g, LATER)

        @pl.when(g == 5 - gx)
        def _():
            for d, i in ((0, 0), (2, 0), (2, 1)):
                arrived(d, i)

        @pl.when(g == 6 + 2 * gx)
        def _():
            arrived(1, 3)

        @pl.when((g == 7) & (gx == 0))
        def _():
            last_gather()

        for first, item in ((1, 1), (2, 4), (3, 5), (4 + 2 * gx, 2), (8 + gx, 3), (12 + 2 * gx, 6), (16 + gx, 7)):
            pl.when(g == first)(functools.partial(take_q, zero + item))

        with jax.named_scope("at"):
            pl.when(t == own)(lambda: both(n, t, m, s, True))
            pl.when(t != own)(lambda: both(n, t, m, s, False))
        pl.when(s == 2 * lax.div(lax.rem(m, 4), 2))(lambda: finish(m))
        return n, t

    def last_gather():
        for d, i in ((0, 2), (2, 2), (2, 3)):
            arrived(d, i)

    at = lax.fori_loop(1, 20, attend, (zero, gx))
    for i in range(CORES):
        weigh(i, at[1], noted(top_s, at[0])[i], noted(keep_s, at[0])[i], held(at[0]))
    finish(at[0])

    for p in range(2):
        with jax.named_scope("wait_o"):
            for k in range(nu):
                pltpu.make_async_copy(os.at[0, 0], og.at[p, k], o_recv.at[p, k]).wait()

        with jax.named_scope("wait_wo"):
            for n in range(slabs):
                load_o(p, n).wait()
        with jax.named_scope("wo"):
            for n in range(slabs):
                more = _dot(og[p, 0], wobuf[p * slabs + n, 0])
                for k in range(1, nu):
                    more += _dot(og[p, k], wobuf[p * slabs + n, k])
                if p == 0:
                    acc[:, n * step : (n + 1) * step] = more + xv[:, n * step : (n + 1) * step].astype(jnp.float32)
                else:
                    y_ref[:, n * step : (n + 1) * step] = (acc[:, n * step : (n + 1) * step] + more).astype(jnp.bfloat16)

    for n in range(nc):
        xx, yy, _ = other(jnp.int32(UNITS[n]))
        for h in range(CORES):
            i = n * CORES + h
            wait = remote(kvs.at[i], kvg.at[me], kv_send.at[i], kv_recv.at[u], dev(xx, yy, h)).wait_send
            if UNITS[n] > 0:
                wait()
            else:
                pl.when(c != h)(wait)
    for i in range(nc):
        for d in range(2):
            passed(d, i).wait_send()
        relayed(i).wait_send()

    def left(n, _):
        for h in range(CORES):
            pl.when(jnp.logical_not(stays(n, h)))(send_q(n, h).wait_send)
        far, h, _ = of(n)
        for i in range(2):
            pl.when((far * 2 + i) * CORES + h != u)(sent(n, i).wait_send)

    lax.fori_loop(0, nu, left, None)
    pl.when(gx == 1)(last_gather)


def solution(mesh):
    total = mesh.shape["sp"]

    def step(x, gain, wq, wk, wv, wo):
        own, dim = x.shape
        nu = wk.shape[1] // HEAD
        side = math.isqrt(total // CORES)
        group = wq.shape[1] // nu
        half = HEAD // 2
        rate = THETA ** (-jnp.arange(half, dtype=jnp.float32) / half)
        rate = jnp.concatenate([rate, rate])[None]
        any_ = pl.BlockSpec(memory_space=pltpu.HBM)
        vmem = pl.BlockSpec(memory_space=pltpu.VMEM)
        low, wide = jnp.bfloat16, jnp.float32
        dma = pltpu.SemaphoreType.DMA
        cols = 2 * HEAD
        step_o = min(dim, 512)
        y = pl.pallas_call(
            functools.partial(_kernel, side),
            out_shape=jax.ShapeDtypeStruct((own, dim), low),
            in_specs=[any_, vmem, vmem, any_, any_, any_, any_],
            out_specs=vmem,
            scratch_shapes=[
                pltpu.VMEM((own, dim), low),
                pltpu.VMEM((own, dim), low),
                pltpu.VMEM((own, HEAD), wide),
                pltpu.VMEM((own, HEAD), wide),
                pltpu.VMEM((SLOTS, dim, group), low),
                pltpu.VMEM((2 * dim // step_o, nu, cols, step_o), low),
                pltpu.VMEM((nu, 2 * HEAD, own), low),
                pltpu.VMEM((total, 2 * HEAD, own), low),
                pltpu.VMEM((nu, 2, own, cols), low),
                pltpu.VMEM((2, nu, own, cols), low),
                pltpu.VMEM((nu, CORES, own, cols), low),
                pltpu.VMEM((2, nu, own, cols), low),
                pltpu.VMEM((own, dim), wide),
                pltpu.VMEM((nu, CORES, cols), wide),
                pltpu.VMEM((nu, CORES, cols), wide),
                pltpu.VMEM((5, CORES, HEAD + 8, cols), wide),
                pltpu.VMEM((CORES, side * CORES * own, cols), wide),
                dma, dma((SLOTS, 2)), dma((2 * dim // step_o,)),
                dma((nu,)), dma((nu,)), dma((3, 4)), dma((3, 4)),
                dma((nu, CORES)), dma((2, nu)), dma((nu, CORES)), dma((2, nu)),
            ],
            compiler_params=pltpu.CompilerParams(collective_id=0, has_side_effects=True, vmem_limit_bytes=VMEM),
        )(x, gain.reshape(-1, HEAD), rate, wq, wk, wv, wo.reshape(nu, 2, cols, dim))
        return y

    tokens, whole = P(("dp", "sp"), None), P(None, None)
    return jax.shard_map(
        step,
        mesh=mesh,
        in_specs=(tokens, P(None), whole, whole, whole, whole),
        out_specs=tokens,
        check_vma=False,
    )
```
